128 devices in a mesh: beam: 16 (over z_lo, y, core), hid: 8 (over x, z_hi).
Axes of the slice: x: 4, y: 4, z: 4 (z_hi: 2, z_lo: 2; z = z_hi * 2 + z_lo), core: 2. Of those that a mesh axis runs over, the one named last changes fastest.
Arguments:
- queries: bfloat16 [1024, 256], P('beam'), may hold values from -6 to 6
- beam_ids: int32 [1024, 256], P('beam'), may hold values from 0 to 262143, as said below
- child_table: bfloat16 [524288, 256], P('beam'), may hold values from -6 to 6
- w_query: bfloat16 [256, 1024], P(None, 'hid'), may hold values from -0.21875 to 0.21875
- w_child: bfloat16 [256, 1024], P(None, 'hid'), may hold values from -0.21875 to 0.21875
- w_cross: bfloat16 [256, 1024], P(None, 'hid'), may hold values from -0.21875 to 0.21875
- bias: float32 [1024], P('hid'), may hold values from -3 to 3
- w_out: float32 [1024], P('hid'), may hold values from -0.1875 to 0.1875
Outputs:
- scores: float32 [1024, 512], P('beam', 'hid')
The draws below stay inside these ranges and needn't reach their ends.
Inputs may be any that keep to these rules, and one draw needn't show every extreme that they name: `beam_ids`: each id b names a node of the current level; its children are rows 2 b and 2 b + 1 of child_table. Among the ids of one index of beam's 64 queries, at most 1536 lie in the rows held by one index of beam (ids r * 16384 to (r + 1) * 16384 - 1 for index r), and in every draw one such index receives exactly 1536 from every index of beam.
All inputs are finite; a program needn't handle non-finite values.
Results may differ from the reference program's by a relative error of at most 0.0019.
Values may be sent and summed in bfloat16 or wider, within the bound.
A program may use at most 128 MiB of HBM per device.

```python
import math
import jax
import jax.numpy as jnp
from jax import lax

E = 256
H = 1024
BEAM = 256
Q_DEV = 64
ROWS_DEV = 32768
QUERIES = 1024
NODES = 524288
CAP = 1536
N_BEAM = 16


def draw_beam_ids(key, part):
    slots = Q_DEV * BEAM
    half = ROWS_DEV // 2
    hottest = jax.random.randint(jax.random.fold_in(key, 11), (), 0, N_BEAM)
    counter = jnp.arange(slots, dtype=jnp.int32)

    def one_block(block_key):
        others = hottest + 1 + (counter - CAP) % (N_BEAM - 1)
        owners = jnp.where(counter < CAP, hottest, others) % N_BEAM
        owners = jax.random.permutation(jax.random.fold_in(block_key, 2), owners)
        offsets = jax.random.randint(jax.random.fold_in(block_key, 3), (slots,), 0, half)
        return (owners * half + offsets).reshape(Q_DEV, BEAM)
    block_keys = jax.random.split(jax.random.fold_in(key, 4), N_BEAM)
    return jax.vmap(one_block)(block_keys).reshape(Q_DEV * N_BEAM, BEAM).astype(jnp.int32)


def block_levels(rng, extent, shards, low, high):
    gain = 1.0
    for position, parts in shards:
        steps = jax.random.uniform(jax.random.fold_in(jax.random.fold_in(rng, 6), position), (parts,), jnp.float32, low / len(shards), high / len(shards))
        gain = gain * jnp.repeat(jnp.exp(steps), extent[position] // parts).reshape((-1,) + (1,) * (len(extent) - 1 - position))
    return gain


def centred(key, extent, deviation, reach, pieces=(), held_as=jnp.bfloat16):
    values = jax.random.normal(key, extent, jnp.float32) * deviation
    if len(pieces) > 0:
        values = block_levels(key, extent, pieces, -0.22, 0.18) * values
    return jnp.clip(values, min=-reach, max=reach).astype(held_as)


def setup_inputs(seed: int = 0) -> dict:
    key_list = jax.random.split(jax.random.key(seed), 9)
    return {
        "queries": centred(key_list[0], (QUERIES, E), 1.0, 6.0, ((0, 16),)),
        "beam_ids": draw_beam_ids(jax.random.fold_in(key_list[8], 71), 0),
        "child_table": centred(key_list[2], (NODES, E), 1.0, 6.0, ((0, 16),)),
        "w_query": centred(key_list[3], (E, H), (3 * E) ** -0.5, 0.21875, ((1, 8),)),
        "w_child": centred(key_list[4], (E, H), (3 * E) ** -0.5, 0.21875, ((1, 8),)),
        "w_cross": centred(key_list[5], (E, H), (3 * E) ** -0.5, 0.21875, ((1, 8),)),
        "bias": centred(key_list[6], (H,), 0.5, 3.0, ((0, 8),), jnp.float32),
        "w_out": centred(key_list[7], (H,), H ** -0.5, 0.1875, ((0, 8),), jnp.float32),
    }


def reference(queries, beam_ids, child_table, w_query, w_child, w_cross, bias, w_out):
    pairs_table = child_table.reshape(NODES // 2, 2 * E)
    qproj = jnp.dot(queries, w_query, preferred_element_type=jnp.float32) + bias
    width = math.gcd(QUERIES, 16)
    count = QUERIES // width

    def score_block(packed):
        ids, qblock, pblock = packed
        rows = pairs_table[ids].reshape(width, 2 * BEAM, E)
        cross = (qblock[:, None, :].astype(jnp.float32) * rows.astype(jnp.float32)).astype(jnp.bfloat16)
        flat_rows = rows.reshape(width * 2 * BEAM, E)
        flat_cross = cross.reshape(width * 2 * BEAM, E)
        pre = jnp.dot(flat_rows, w_child, preferred_element_type=jnp.float32) + jnp.dot(flat_cross, w_cross, preferred_element_type=jnp.float32)
        pre = pre.reshape(width, 2 * BEAM, H) + pblock[:, None, :]
        return jnp.sum(jnp.maximum(pre, 0.0) * w_out, axis=-1)

    result = lax.map(score_block, (beam_ids.reshape(count, width, BEAM), queries.reshape(count, width, E), qproj.reshape(count, width, H)))
    return result.reshape(QUERIES, 2 * BEAM)
```

```python
import functools
import math

import jax
import jax.numpy as jnp
from jax import lax
from jax.experimental import pallas as pl
from jax.experimental.pallas import tpu as pltpu
from jax.sharding import PartitionSpec as P

F32, BF16, I32 = jnp.float32, jnp.bfloat16, jnp.int32
NT = (((1,), (1,)), ((), ()))
TN = (((0,), (0,)), ((), ()))


def iota(shape, dim):
    return lax.broadcasted_iota(I32, shape, dim)


def route(h, nbeam, share, half, ids_ref, req_ref, rank_ref, a_ref, c_ref, v0_ref, v1_ref, q_ref):
    qd, width = ids_ref.shape
    lo = ids_ref[:, :128]
    hi = ids_ref[:, 128:]
    ids = jnp.concatenate([lo, hi], axis=0)
    rows = ids.shape[0]
    owner = ids // half
    before_lane = (iota((128, 128), 0) < iota((128, 128), 1)).astype(BF16)
    ones = jnp.ones((128, 128), BF16)
    both = jnp.concatenate([before_lane, ones], axis=1)
    before_row = (iota((rows, rows), 1) < iota((rows, rows), 0)).astype(BF16)
    rank = jnp.zeros((rows, 128), F32)
    for o in range(nbeam):
        hit = owner == o
        counts = jnp.dot(hit.astype(BF16), both, preferred_element_type=F32)
        above = jnp.dot(before_row, counts[:, 128:].astype(BF16), preferred_element_type=F32)
        rank = rank + jnp.where(hit, counts[:, :128] + above, 0.0)
    rank = rank.astype(I32)
    rank = jnp.concatenate([rank[:qd], rank[qd:]], axis=1)
    rank_ref[...] = rank
    ids = ids_ref[...]
    owner = ids // half
    offset = ids - owner * half
    local = rank - h * share
    place = owner * 256 + local
    inside = (local >= 0) & (local < share)
    a_ref[...] = jnp.where(inside, place // 128, -1)
    c_ref[...] = place % 128
    v0_ref[...] = (offset % 128).astype(F32)
    v1_ref[...] = (offset // 128).astype(F32)
    q_ref[...] = iota((qd, width), 0).astype(F32)
    na = 2 * nbeam
    arow = iota((na, width), 0)
    crow = iota((128, width), 0)

    def step(r, total):
        one = pl.ds(r, 1)
        hit = arow == a_ref[one, :]
        left = jnp.concatenate([jnp.where(hit, ref[one, :], 0.0) for ref in (v0_ref, v1_ref, q_ref)], axis=0)
        right = (crow == c_ref[one, :]).astype(F32)
        return total + lax.dot_general(left.astype(BF16), right.astype(BF16), NT, preferred_element_type=F32)

    table = lax.fori_loop(0, qd, step, jnp.zeros((3 * na, 128), F32), unroll=8).astype(I32)
    offs = table[:na] + 128 * table[na : 2 * na]
    qs = table[2 * na :]
    for o in range(nbeam):
        req_ref[o, 0:2, :] = offs[2 * o : 2 * o + 2]
        req_ref[o, 2:4, :] = qs[2 * o : 2 * o + 2]


def table_copies(table_ref, buf_ref, sems):
    groups = table_ref.shape[0] // 8
    width = table_ref.shape[1]
    src = table_ref.reshape(groups, 8, width)
    dst = buf_ref.reshape(groups, 4, 2, width)
    return [pltpu.make_async_copy(src.at[:, 2 * p : 2 * p + 2, :], dst.at[:, p], sems.at[p]) for p in range(4)]


def gather(share, off_ref, buf_ref, rows_ref, first, count):
    def one(b, _):
        for k in range(share):
            rows_ref[b * share + k] = buf_ref[off_ref[first + b, k // 128, k % 128]]
        return 0

    lax.fori_loop(0, count, one, 0)


def split2(x):
    hi = x.astype(BF16)
    return hi, (x - hi.astype(F32)).astype(BF16)


def score(share, b0, nb, qd, req_ref, rows_ref, queries_ref, wq_ref, wc_ref, wx_ref, vec_ref, out_ref):
    shards = wq_ref.shape[0]
    width = queries_ref.shape[1]
    m = nb * 2 * share
    qrows = []
    dup = (iota((2 * share, share), 0) // 2 == iota((2 * share, share), 1)).astype(BF16)
    for i in range(nb):
        b = b0 + i
        qvec = jnp.concatenate([req_ref[b, 2:3, :], req_ref[b, 3:4, : share - 128]], axis=1)
        oht = (iota((qd, share), 0) == qvec).astype(F32).astype(BF16)
        qb = queries_ref[pl.ds(pl.multiple_of(b * qd, qd), qd), :]
        qrow = lax.dot_general(oht, qb, TN, preferred_element_type=F32).astype(BF16)
        qrows.append(jnp.dot(dup, qrow, preferred_element_type=F32).astype(BF16))
    qrow = jnp.concatenate(qrows, axis=0) if nb > 1 else qrows[0]
    child = rows_ref[...].reshape(m, width)
    cross = child * qrow
    acc = jnp.zeros((m, 128), F32)
    for n in range(0, shards, 2):
        pair = lambda ref: jnp.concatenate([ref[n], ref[n + 1]], axis=1)
        pre = jnp.dot(child, pair(wc_ref), preferred_element_type=F32)
        pre += jnp.dot(cross, pair(wx_ref), preferred_element_type=F32)
        pre += jnp.dot(qrow, pair(wq_ref), preferred_element_type=F32)
        for j in range(2):
            part = pre[:, 128 * j : 128 * j + 128]
            acc += jnp.maximum(part + vec_ref[n + j, 0:1, :], 0.0) * vec_ref[n + j, 1:2, :]
    total = acc.T
    total = jnp.sum(total, axis=0, keepdims=True)
    for i in range(nb):
        for t in range(2 * share // 128):
            lo = i * 2 * share + t * 128
            out_ref[b0 + i, t : t + 1, :] = total[:, lo : lo + 128]


def unpermute(h, nhid, nbeam, share, half, ids_ref, rank_ref, sall_ref, out_ref):
    qd, width = ids_ref.shape
    per = width // nhid

    def own(x):
        mine = jnp.zeros((qd, per), I32)
        for k in range(nhid):
            mine = jnp.where(h == k, x[:, k * per : (k + 1) * per], mine)
        return jnp.concatenate([mine[8 * g : 8 * g + 8] for g in range(qd // 8)], axis=1)

    owner = own(ids_ref[...]) // half
    rank = own(rank_ref[...])
    chunk = rank // share
    local = rank - chunk * share
    tiles = 2 * share // 128
    row = (chunk * nbeam + owner) * tiles + local // 64
    lane = (local % 64) * 2
    nrows = nhid * nbeam * tiles
    scores = sall_ref[...].reshape(nrows, 128).T
    hi, lo = split2(scores)
    parts = jnp.concatenate([hi, lo], axis=0)
    lanes = lane.shape[1]
    rio = iota((nrows, lanes), 0)
    cio = iota((128, lanes), 0)
    evens, odds = [], []
    for i in range(8):
        onehot = (rio == row[i : i + 1]).astype(F32).astype(BF16)
        got = jnp.dot(parts, onehot, preferred_element_type=F32)
        got = got[:128] + got[128:]
        evens.append(jnp.sum(jnp.where(cio == lane[i : i + 1], got, 0.0), axis=0, keepdims=True))
        odds.append(jnp.sum(jnp.where(cio == lane[i : i + 1] + 1, got, 0.0), axis=0, keepdims=True))
    even = jnp.concatenate(split2(jnp.concatenate(evens, axis=0)), axis=0)
    odd = jnp.concatenate(split2(jnp.concatenate(odds, axis=0)), axis=0)
    n = iota((lanes, 2 * lanes), 1)
    k = iota((lanes, 2 * lanes), 0)
    mixed = jnp.dot(even, (n == 2 * k).astype(BF16), preferred_element_type=F32)
    mixed += jnp.dot(odd, (n == 2 * k + 1).astype(BF16), preferred_element_type=F32)
    mixed = mixed[:8] + mixed[8:]
    for g in range(qd // 8):
        out_ref[8 * g : 8 * g + 8, :] = mixed[:, 2 * per * g : 2 * per * (g + 1)]


BEAM, HID = 16, 8
MESH = pl.DeviceIdType.MESH


def peer_beam(b, j):
    return lax.rem(b + j, BEAM)


def peer_hid(h, j):
    return lax.rem(h + j, HID)


def entry_barrier(b, h):
    barrier = pltpu.get_barrier_semaphore()

    def beam(j, _):
        pl.semaphore_signal(barrier, inc=1, device_id=(peer_beam(b, j), h), device_id_type=MESH)
        return 0

    def hid(j, _):
        pl.semaphore_signal(barrier, inc=1, device_id=(b, peer_hid(h, j)), device_id_type=MESH)
        return 0

    lax.fori_loop(1, BEAM, beam, 0)
    lax.fori_loop(1, HID, hid, 0)
    pl.semaphore_wait(barrier, BEAM + HID - 2)


def remote(src, dst, send, recv, device):
    return pltpu.make_async_remote_copy(
        src_ref=src, dst_ref=dst, send_sem=send, recv_sem=recv, device_id=device, device_id_type=MESH
    )


def exchange_kernel(req, queries, wq, wc, wx, vec, req_all, q_all, wq_all, wc_all, wx_all, vec_all, bsend, brecv, hsend, hrecv):
    b, h = lax.axis_index("beam"), lax.axis_index("hid")
    qd = queries.shape[0]
    entry_barrier(b, h)
    spread = ((wq, wq_all), (wc, wc_all), (wx, wx_all), (vec, vec_all))

    def rows(i):
        return pl.ds(pl.multiple_of(i * qd, qd), qd)

    def beam_copies(to, sem, slot):
        device = (to, h)
        return (
            remote(req.at[to], req_all.at[slot], bsend.at[0, sem], brecv.at[0, slot], device),
            remote(queries, q_all.at[rows(slot)], bsend.at[1, sem], brecv.at[1, slot], device),
        )

    def hid_copies(to, sem, slot):
        return [
            remote(src, dst.at[slot], hsend.at[i, sem], hrecv.at[i, slot], (b, to))
            for i, (src, dst) in enumerate(spread)
        ]

    def start_hid(j, _):
        for copy in hid_copies(peer_hid(h, j), peer_hid(h, j), h):
            copy.start()
        return 0

    def start_beam(j, _):
        for copy in beam_copies(peer_beam(b, j), peer_beam(b, j), b):
            copy.start()
        return 0

    lax.fori_loop(1, BEAM, start_beam, 0)
    lax.fori_loop(1, HID, start_hid, 0)
    req_all[pl.ds(b, 1)] = req[pl.ds(b, 1)]
    q_all[rows(b), :] = queries[...]
    for src, dst in spread:
        dst[h] = src[...]

    def wait_beam(j, _):
        peer = peer_beam(b, j)
        for copy in beam_copies(peer, peer, peer):
            copy.wait()
        return 0

    def wait_hid(j, _):
        peer = peer_hid(h, j)
        for copy in hid_copies(peer, peer, peer):
            copy.wait()
        return 0

    lax.fori_loop(1, BEAM, wait_beam, 0)
    lax.fori_loop(1, HID, wait_hid, 0)


def return_kernel(scores, sall, bsend, brecv, hsend, hrecv):
    b, h = lax.axis_index("beam"), lax.axis_index("hid")
    entry_barrier(b, h)

    def back(to, slot):
        return remote(scores.at[to], sall.at[h, slot], bsend.at[to], brecv.at[slot], (to, h))

    def spread(to, slot):
        return remote(sall.at[slot], sall.at[slot], hsend.at[to], hrecv.at[slot], (b, to))

    def start_back(j, _):
        back(peer_beam(b, j), b).start()
        return 0

    def wait_back(j, _):
        back(peer_beam(b, j), peer_beam(b, j)).wait()
        return 0

    def start_spread(j, _):
        spread(peer_hid(h, j), h).start()
        return 0

    def wait_spread(j, _):
        spread(peer_hid(h, j), peer_hid(h, j)).wait()
        return 0

    lax.fori_loop(1, BEAM, start_back, 0)
    sall[h, pl.ds(b, 1)] = scores[pl.ds(b, 1)]
    lax.fori_loop(1, BEAM, wait_back, 0)
    lax.fori_loop(1, HID, start_spread, 0)
    lax.fori_loop(1, HID, wait_spread, 0)


VM = pl.BlockSpec(memory_space=pltpu.VMEM)
SM = pl.BlockSpec(memory_space=pltpu.SMEM)
ANY = pl.BlockSpec(memory_space=pl.ANY)


def shape(dims, dtype):
    return jax.ShapeDtypeStruct(dims, dtype)


def dma(*dims):
    return pltpu.SemaphoreType.DMA(dims)


def shards(queries, beam_ids, child_table, w_query, w_child, w_cross, bias, w_out):
    qd, width = beam_ids.shape
    embed = queries.shape[1]
    half = child_table.shape[0] // 2
    hid_dev = w_query.shape[1]
    share = 3 * qd * width // (2 * BEAM * HID)
    nb = 2

    def route_kernel(ids, req, rank, *scratch):
        route(lax.axis_index("hid"), BEAM, share, half, ids, req, rank, *scratch)

    req, rank = pl.pallas_call(
        route_kernel,
        out_shape=(shape((BEAM, 4, 128), I32), shape((qd, width), I32)),
        in_specs=[VM],
        out_specs=(VM, VM),
        scratch_shapes=[pltpu.VMEM((qd, width), I32)] * 2 + [pltpu.VMEM((qd, width), F32)] * 3,
        name="route",
    )(beam_ids)

    vec = jnp.stack([bias, w_out])
    req_all, q_all, wq_all, wc_all, wx_all, vec_all = pl.pallas_call(
        exchange_kernel,
        out_shape=(
            shape((BEAM, 4, 128), I32),
            shape((BEAM * qd, embed), BF16),
            *[shape((HID, embed, hid_dev), BF16)] * 3,
            shape((HID, 2, hid_dev), F32),
        ),
        in_specs=[VM] * 6,
        out_specs=(VM,) * 6,
        scratch_shapes=[dma(2, BEAM), dma(2, BEAM), dma(4, HID), dma(4, HID)],
        compiler_params=pltpu.CompilerParams(collective_id=0, has_side_effects=True),
        name="exchange",
    )(req, queries, w_query, w_child, w_cross, vec)

    def score_kernel(req, off, table, queries, wq, wc, wx, vec, out, buf, rows, sems):
        copies = table_copies(table, buf, sems)
        for copy in copies:
            copy.start()
        for copy in copies:
            copy.wait()

        def step(i, _):
            gather(share, off, buf, rows, i * nb, nb)
            score(share, i * nb, nb, qd, req, rows, queries, wq, wc, wx, vec, out)
            return 0

        lax.fori_loop(0, BEAM // nb, step, 0)

    scores = pl.pallas_call(
        score_kernel,
        out_shape=shape((BEAM, 3, 128), F32),
        in_specs=[VM, SM, ANY, VM, VM, VM, VM, VM],
        out_specs=VM,
        scratch_shapes=[
            pltpu.VMEM((half, 2, embed), BF16),
            pltpu.VMEM((nb * share, 2, embed), BF16),
            dma(4),
        ],
        compiler_params=pltpu.CompilerParams(vmem_limit_bytes=56 * 2**20),
        name="score",
    )(req_all, req_all, child_table, q_all, wq_all, wc_all, wx_all, vec_all)

    sall = pl.pallas_call(
        return_kernel,
        out_shape=shape((HID, BEAM, 3, 128), F32),
        in_specs=[VM],
        out_specs=VM,
        scratch_shapes=[dma(BEAM), dma(BEAM), dma(HID), dma(HID)],
        compiler_params=pltpu.CompilerParams(collective_id=1, has_side_effects=True),
        name="give_back",
    )(scores)

    def place_kernel(ids, rank, sall, out):
        unpermute(lax.axis_index("hid"), HID, BEAM, share, half, ids, rank, sall, out)

    return pl.pallas_call(
        place_kernel,
        out_shape=shape((qd, 2 * width // HID), F32),
        in_specs=[VM] * 3,
        out_specs=VM,
        name="place",
    )(beam_ids, rank, sall)


def solution(mesh):
    return jax.shard_map(
        shards,
        mesh=mesh,
        in_specs=(
            P("beam", None),
            P("beam", None),
            P("beam", None),
            P(None, "hid"),
            P(None, "hid"),
            P(None, "hid"),
            P("hid"),
            P("hid"),
        ),
        out_specs=P("beam", "hid"),
        check_vma=False,
    )
```

```python
import functools
import math

import jax
import jax.numpy as jnp
from jax import lax
from jax.experimental import pallas as pl
from jax.experimental.pallas import tpu as pltpu
from jax.sharding import PartitionSpec as P

F32, BF16, I32 = jnp.float32, jnp.bfloat16, jnp.int32
NT = (((1,), (1,)), ((), ()))
TN = (((0,), (0,)), ((), ()))


def iota(shape, dim):
    return lax.broadcasted_iota(I32, shape, dim)


def route(h, nbeam, share, half, ids_ref, req_ref, rank_ref, a_ref, c_ref, v0_ref, v1_ref, q_ref):
    qd, width = ids_ref.shape
    lo = ids_ref[:, :128]
    hi = ids_ref[:, 128:]
    ids = jnp.concatenate([lo, hi], axis=0)
    rows = ids.shape[0]
    owner = ids // half
    before_lane = (iota((128, 128), 0) < iota((128, 128), 1)).astype(BF16)
    ones = jnp.ones((128, 128), BF16)
    both = jnp.concatenate([before_lane, ones], axis=1)
    before_row = (iota((rows, rows), 1) < iota((rows, rows), 0)).astype(BF16)
    rank = jnp.zeros((rows, 128), F32)
    for o in range(nbeam):
        hit = owner == o
        counts = jnp.dot(hit.astype(BF16), both, preferred_element_type=F32)
        above = jnp.dot(before_row, counts[:, 128:].astype(BF16), preferred_element_type=F32)
        rank = rank + jnp.where(hit, counts[:, :128] + above, 0.0)
    rank = rank.astype(I32)
    rank = jnp.concatenate([rank[:qd], rank[qd:]], axis=1)
    rank_ref[...] = rank
    ids = ids_ref[...]
    owner = ids // half
    offset = ids - owner * half
    local = rank - h * share
    place = owner * 256 + local
    inside = (local >= 0) & (local < share)
    a_ref[...] = jnp.where(inside, place // 128, -1)
    c_ref[...] = place % 128
    v0_ref[...] = (offset % 128).astype(F32)
    v1_ref[...] = (offset // 128).astype(F32)
    q_ref[...] = iota((qd, width), 0).astype(F32)
    na = 2 * nbeam
    arow = iota((na, width), 0)
    crow = iota((128, width), 0)

    def step(r, total):
        one = pl.ds(r, 1)
        hit = arow == a_ref[one, :]
        left = jnp.concatenate([jnp.where(hit, ref[one, :], 0.0) for ref in (v0_ref, v1_ref, q_ref)], axis=0)
        right = (crow == c_ref[one, :]).astype(F32)
        return total + lax.dot_general(left.astype(BF16), right.astype(BF16), NT, preferred_element_type=F32)

    table = lax.fori_loop(0, qd, step, jnp.zeros((3 * na, 128), F32), unroll=8).astype(I32)
    offs = table[:na] + 128 * table[na : 2 * na]
    qs = table[2 * na :]
    for o in range(nbeam):
        req_ref[o, 0:2, :] = offs[2 * o : 2 * o + 2]
        req_ref[o, 2:4, :] = qs[2 * o : 2 * o + 2]


def table_copies(table_ref, buf_ref, sems):
    groups = table_ref.shape[0] // 8
    width = table_ref.shape[1]
    src = table_ref.reshape(groups, 8, width)
    dst = buf_ref.reshape(groups, 4, 2, width)
    return [pltpu.make_async_copy(src.at[:, 2 * p : 2 * p + 2, :], dst.at[:, p], sems.at[p]) for p in range(4)]


def gather(share, off_ref, buf_ref, rows_ref, first, count):
    def one(b, _):
        for k in range(share):
            rows_ref[b * share + k] = buf_ref[off_ref[first + b, k // 128, k % 128]]
        return 0

    lax.fori_loop(0, count, one, 0)


def split2(x):
    hi = x.astype(BF16)
    return hi, (x - hi.astype(F32)).astype(BF16)


def score(share, b0, nb, qd, req_ref, rows_ref, queries_ref, wq_ref, wc_ref, wx_ref, vec_ref, out_ref):
    shards = wq_ref.shape[0]
    width = queries_ref.shape[1]
    m = nb * 2 * share
    qrows = []
    dup = (iota((2 * share, share), 0) // 2 == iota((2 * share, share), 1)).astype(BF16)
    for i in range(nb):
        b = b0 + i
        qvec = jnp.concatenate([req_ref[b, 2:3, :], req_ref[b, 3:4, : share - 128]], axis=1)
        oht = (iota((qd, share), 0) == qvec).astype(F32).astype(BF16)
        qb = queries_ref[pl.ds(pl.multiple_of(b * qd, qd), qd), :]
        qrow = lax.dot_general(oht, qb, TN, preferred_element_type=F32).astype(BF16)
        qrows.append(jnp.dot(dup, qrow, preferred_element_type=F32).astype(BF16))
    qrow = jnp.concatenate(qrows, axis=0) if nb > 1 else qrows[0]
    child = rows_ref[...].reshape(m, width)
    cross = child * qrow
    acc = jnp.zeros((m, 128), F32)
    for n in range(0, shards, 2):
        pair = lambda ref: jnp.concatenate([ref[n], ref[n + 1]], axis=1)
        pre = jnp.dot(child, pair(wc_ref), preferred_element_type=F32)
        pre += jnp.dot(cross, pair(wx_ref), preferred_element_type=F32)
        pre += jnp.dot(qrow, pair(wq_ref), preferred_element_type=F32)
        for j in range(2):
            part = pre[:, 128 * j : 128 * j + 128]
            acc += jnp.maximum(part + vec_ref[n + j, 0:1, :], 0.0) * vec_ref[n + j, 1:2, :]
    total = acc.T
    total = jnp.sum(total, axis=0, keepdims=True)
    for i in range(nb):
        for t in range(2 * share // 128):
            lo = i * 2 * share + t * 128
            out_ref[b0 + i, t : t + 1, :] = total[:, lo : lo + 128]


def unpermute(h, nhid, nbeam, share, half, ids_ref, rank_ref, sall_ref, out_ref):
    qd, width = ids_ref.shape
    per = width // nhid

    def own(x):
        mine = jnp.zeros((qd, per), I32)
        for k in range(nhid):
            mine = jnp.where(h == k, x[:, k * per : (k + 1) * per], mine)
        return jnp.concatenate([mine[8 * g : 8 * g + 8] for g in range(qd // 8)], axis=1)

    owner = own(ids_ref[...]) // half
    rank = own(rank_ref[...])
    chunk = rank // share
    local = rank - chunk * share
    tiles = 2 * share // 128
    row = (chunk * nbeam + owner) * tiles + local // 64
    lane = (local % 64) * 2
    nrows = nhid * nbeam * tiles
    scores = sall_ref[...].reshape(nrows, 128).T
    hi, lo = split2(scores)
    parts = jnp.concatenate([hi, lo], axis=0)
    lanes = lane.shape[1]
    rio = iota((nrows, lanes), 0)
    cio = iota((128, lanes), 0)
    evens, odds = [], []
    for i in range(8):
        onehot = (rio == row[i : i + 1]).astype(F32).astype(BF16)
        got = jnp.dot(parts, onehot, preferred_element_type=F32)
        got = got[:128] + got[128:]
        evens.append(jnp.sum(jnp.where(cio == lane[i : i + 1], got, 0.0), axis=0, keepdims=True))
        odds.append(jnp.sum(jnp.where(cio == lane[i : i + 1] + 1, got, 0.0), axis=0, keepdims=True))
    even = jnp.concatenate(split2(jnp.concatenate(evens, axis=0)), axis=0)
    odd = jnp.concatenate(split2(jnp.concatenate(odds, axis=0)), axis=0)
    n = iota((lanes, 2 * lanes), 1)
    k = iota((lanes, 2 * lanes), 0)
    mixed = jnp.dot(even, (n == 2 * k).astype(BF16), preferred_element_type=F32)
    mixed += jnp.dot(odd, (n == 2 * k + 1).astype(BF16), preferred_element_type=F32)
    mixed = mixed[:8] + mixed[8:]
    for g in range(qd // 8):
        out_ref[8 * g : 8 * g + 8, :] = mixed[:, 2 * per * g : 2 * per * (g + 1)]


BEAM, HID = 16, 8
MESH = pl.DeviceIdType.MESH
VM = pl.BlockSpec(memory_space=pltpu.VMEM)
ANY = pl.BlockSpec(memory_space=pl.ANY)


def shape(dims, dtype):
    return jax.ShapeDtypeStruct(dims, dtype)


def dma(*dims):
    return pltpu.SemaphoreType.DMA(dims)


def remote(src, dst, send, recv, device):
    return pltpu.make_async_remote_copy(
        src_ref=src, dst_ref=dst, send_sem=send, recv_sem=recv, device_id=device, device_id_type=MESH
    )


def loop(lo, hi, body):
    def step(i, _):
        body(i)
        return 0

    lax.fori_loop(lo, hi, step, 0)


def front_kernel(
    share,
    ids,
    queries,
    wq,
    wc,
    wx,
    bias,
    w_out,
    table,
    rank,
    req_all,
    q_all,
    w_all,
    vec_all,
    buf,
    req,
    a_ref,
    c_ref,
    v0_ref,
    v1_ref,
    qi_ref,
    table_sem,
    own_sem,
    rsend,
    rrecv,
    qsend,
    qrecv,
    vsend,
    vrecv,
    wsend,
    wrecv,
    psend,
    precv,
):
    b, h = lax.axis_index("beam"), lax.axis_index("hid")
    core = lax.rem(b, 2)
    mate = b + 1 - 2 * core
    z = lax.rem(h, 2)
    across = h + 1 - 2 * z
    qd = ids.shape[0]
    half = table.shape[0] // 2
    depth = w_all.shape[2] // 2

    def beam_peer(j):
        return lax.rem(b + j, BEAM)

    def hid_peer(j):
        return lax.rem(h + j, HID)

    def x_peer(j):
        return lax.rem(h + 2 * j, HID)

    barrier = pltpu.get_barrier_semaphore()
    loop(1, BEAM, lambda j: pl.semaphore_signal(barrier, inc=1, device_id=(beam_peer(j), h), device_id_type=MESH))
    loop(1, HID, lambda j: pl.semaphore_signal(barrier, inc=1, device_id=(b, hid_peer(j)), device_id_type=MESH))

    def q_rows(i):
        return pl.ds(pl.multiple_of(i * qd, qd), qd)

    own = [
        pltpu.make_async_copy(src, w_all.at[h, i], own_sem.at[i]) for i, src in enumerate((wq, wc, wx))
    ]
    own.append(pltpu.make_async_copy(queries, q_all.at[q_rows(b), :], own_sem.at[3]))
    own.append(pltpu.make_async_copy(bias, vec_all.at[h, 0:1, :], own_sem.at[4]))
    own.append(pltpu.make_async_copy(w_out, vec_all.at[h, 1:2, :], own_sem.at[5]))
    for copy in own:
        copy.start()
    pulls = table_copies(table, buf, table_sem)
    for copy in pulls:
        copy.start()
    for copy in own:
        copy.wait()
    pl.semaphore_wait(barrier, BEAM + HID - 2)

    def piece(shard, part):
        return w_all.at[shard, :, pl.ds(pl.multiple_of(part * depth, depth), depth), :]

    def w_copy(shard, to, slot):
        return remote(piece(shard, core), piece(shard, core), wsend.at[slot], wrecv.at[shard], (b, to))

    def mate_copy(shard):
        return remote(piece(shard, core), piece(shard, core), psend.at[shard], precv.at[shard], (mate, h))

    def mate_arrival(shard):
        other = piece(shard, 1 - core)
        return remote(other, other, psend.at[shard], precv.at[shard], (mate, h))

    def q_copy(to, slot):
        return remote(q_all.at[q_rows(slot), :], q_all.at[q_rows(slot), :], qsend.at[to], qrecv.at[slot], (to, h))

    def v_copy(to, slot):
        return remote(vec_all.at[slot], vec_all.at[slot], vsend.at[to], vrecv.at[slot], (b, to))

    def r_copy(to, slot):
        return remote(req.at[to], req_all.at[slot], rsend.at[to], rrecv.at[slot], (to, h))

    w_copy(h, across, 0).start()
    for j in range(1, 4):
        w_copy(h, x_peer(j), j).start()
    loop(1, HID, lambda j: v_copy(hid_peer(j), h).start())
    loop(1, BEAM, lambda j: q_copy(beam_peer(j), b).start())

    route(h, BEAM, share, half, ids, req, rank, a_ref, c_ref, v0_ref, v1_ref, qi_ref)
    loop(1, BEAM, lambda j: r_copy(beam_peer(j), b).start())
    req_all[pl.ds(b, 1)] = req[pl.ds(b, 1)]

    w_copy(across, across, 0).wait_recv()
    for j in range(1, 4):
        w_copy(across, x_peer(j), 3 + j).start()
    mate_copy(across).start()

    loop(1, BEAM, lambda j: r_copy(beam_peer(j), beam_peer(j)).wait_recv())
    for copy in pulls:
        copy.wait()

    for j in range(1, 4):
        for zz in (h, across):
            shard = lax.rem(zz + 2 * j, HID)
            w_copy(shard, shard, 0).wait_recv()
            mate_copy(shard).start()
    loop(1, BEAM, lambda j: q_copy(beam_peer(j), beam_peer(j)).wait_recv())
    loop(1, HID, lambda j: v_copy(hid_peer(j), hid_peer(j)).wait_recv())
    loop(1, HID, lambda j: mate_arrival(hid_peer(j)).wait_recv())

    w_copy(h, across, 0).wait_send()
    for j in range(1, 4):
        w_copy(h, x_peer(j), j).wait_send()
        w_copy(across, x_peer(j), 3 + j).wait_send()
    loop(1, BEAM, lambda j: q_copy(beam_peer(j), b).wait_send())
    loop(1, BEAM, lambda j: r_copy(beam_peer(j), b).wait_send())
    loop(1, HID, lambda j: v_copy(hid_peer(j), h).wait_send())
    loop(1, HID, lambda j: mate_copy(hid_peer(j)).wait_send())


def back_kernel(scores, sall, bsend, brecv, hsend, hrecv):
    b, h = lax.axis_index("beam"), lax.axis_index("hid")

    def beam_peer(j):
        return lax.rem(b + j, BEAM)

    def hid_peer(j):
        return lax.rem(h + j, HID)

    barrier = pltpu.get_barrier_semaphore()
    loop(1, BEAM, lambda j: pl.semaphore_signal(barrier, inc=1, device_id=(beam_peer(j), h), device_id_type=MESH))
    loop(1, HID, lambda j: pl.semaphore_signal(barrier, inc=1, device_id=(b, hid_peer(j)), device_id_type=MESH))
    pl.semaphore_wait(barrier, BEAM + HID - 2)

    def back(to, slot):
        return remote(scores.at[to], sall.at[h, slot], bsend.at[to], brecv.at[slot], (to, h))

    def spread(to, slot):
        return remote(sall.at[slot], sall.at[slot], hsend.at[to], hrecv.at[slot], (b, to))

    loop(1, BEAM, lambda j: back(beam_peer(j), b).start())
    sall[h, pl.ds(b, 1)] = scores[pl.ds(b, 1)]
    loop(1, BEAM, lambda j: back(beam_peer(j), beam_peer(j)).wait_recv())
    loop(1, HID, lambda j: spread(hid_peer(j), h).start())
    loop(1, BEAM, lambda j: back(beam_peer(j), b).wait_send())
    loop(1, HID, lambda j: spread(hid_peer(j), h).wait_send())
    loop(1, HID, lambda j: spread(hid_peer(j), hid_peer(j)).wait_recv())


def score_kernel(share, nb, qd, req, off, queries, w_all, vec, buf, scores, rows):
    def step(i):
        gather(share, off, buf, rows, i * nb, nb)
        score(share, i * nb, nb, qd, req, rows, queries, w_all.at[:, 0], w_all.at[:, 1], w_all.at[:, 2], vec, scores)

    loop(0, BEAM // nb, step)


def shards(queries, beam_ids, child_table, w_query, w_child, w_cross, bias, w_out):
    qd, width = beam_ids.shape
    embed = queries.shape[1]
    half = child_table.shape[0] // 2
    hid_dev = w_query.shape[1]
    share = 3 * qd * width // (2 * BEAM * HID)
    nb = 4
    ints = pltpu.VMEM((qd, width), I32)
    floats = pltpu.VMEM((qd, width), F32)

    rank, req_all, q_all, w_all, vec_all, buf = pl.pallas_call(
        functools.partial(front_kernel, share),
        out_shape=(
            shape((qd, width), I32),
            shape((BEAM, 4, 128), I32),
            pltpu.VMEM((BEAM * qd, embed), BF16),
            pltpu.VMEM((HID, 3, embed, hid_dev), BF16),
            pltpu.VMEM((HID, 2, hid_dev), F32),
            pltpu.VMEM((half, 2, embed), BF16),
        ),
        in_specs=[VM] + [ANY] * 7,
        out_specs=(VM,) * 6,
        scratch_shapes=[
            pltpu.VMEM((BEAM, 4, 128), I32),
            ints,
            ints,
            floats,
            floats,
            floats,
            dma(4),
            dma(6),
            *[dma(BEAM)] * 4,
            *[dma(HID)] * 2,
            dma(7),
            dma(HID),
            *[dma(HID)] * 2,
        ],
        compiler_params=pltpu.CompilerParams(collective_id=0, has_side_effects=True, vmem_limit_bytes=6 * 2**20),
        name="front",
    )(beam_ids, queries, w_query, w_child, w_cross, bias.reshape(1, -1), w_out.reshape(1, -1), child_table)

    scores = pl.pallas_call(
        functools.partial(score_kernel, share, nb, qd),
        out_shape=shape((BEAM, 3, 128), F32),
        in_specs=[VM, pl.BlockSpec(memory_space=pltpu.SMEM)] + [VM] * 4,
        out_specs=VM,
        scratch_shapes=[pltpu.VMEM((nb * share, 2, embed), BF16)],
        compiler_params=pltpu.CompilerParams(vmem_limit_bytes=20 * 2**20),
        name="score",
    )(req_all, req_all, q_all, w_all, vec_all, buf)

    sall = pl.pallas_call(
        back_kernel,
        out_shape=shape((HID, BEAM, 3, 128), F32),
        in_specs=[VM],
        out_specs=VM,
        scratch_shapes=[dma(BEAM), dma(BEAM), dma(HID), dma(HID)],
        compiler_params=pltpu.CompilerParams(collective_id=1, has_side_effects=True),
        name="give_back",
    )(scores)

    def place_kernel(ids, rank, sall, out):
        unpermute(lax.axis_index("hid"), HID, BEAM, share, half, ids, rank, sall, out)

    return pl.pallas_call(
        place_kernel,
        out_shape=shape((qd, 2 * width // HID), F32),
        in_specs=[VM] * 3,
        out_specs=VM,
        name="place",
    )(beam_ids, rank, sall)


def solution(mesh):
    return jax.shard_map(
        shards,
        mesh=mesh,
        in_specs=(
            P("beam", None),
            P("beam", None),
            P("beam", None),
            P(None, "hid"),
            P(None, "hid"),
            P(None, "hid"),
            P("hid"),
            P("hid"),
        ),
        out_specs=P("beam", "hid"),
        check_vma=False,
    )
```

```python
import functools
import math

import jax
import jax.numpy as jnp
from jax import lax
from jax.experimental import pallas as pl
from jax.experimental.pallas import tpu as pltpu
from jax.sharding import PartitionSpec as P

F32, BF16, I32 = jnp.float32, jnp.bfloat16, jnp.int32
NT = (((1,), (1,)), ((), ()))
TN = (((0,), (0,)), ((), ()))


def iota(shape, dim):
    return lax.broadcasted_iota(I32, shape, dim)


def route(h, nbeam, share, half, ids_ref, req_ref, rank_ref, a_ref, c_ref, v0_ref, v1_ref, q_ref):
    qd, width = ids_ref.shape
    lo = ids_ref[:, :128]
    hi = ids_ref[:, 128:]
    ids = jnp.concatenate([lo, hi], axis=0)
    rows = ids.shape[0]
    owner = ids // half
    before_lane = (iota((128, 128), 0) < iota((128, 128), 1)).astype(BF16)
    ones = jnp.ones((128, 128), BF16)
    both = jnp.concatenate([before_lane, ones], axis=1)
    before_row = (iota((rows, rows), 1) < iota((rows, rows), 0)).astype(BF16)
    rank = jnp.zeros((rows, 128), F32)
    for o in range(nbeam):
        hit = owner == o
        counts = jnp.dot(hit.astype(BF16), both, preferred_element_type=F32)
        above = jnp.dot(before_row, counts[:, 128:].astype(BF16), preferred_element_type=F32)
        rank = rank + jnp.where(hit, counts[:, :128] + above, 0.0)
    rank = rank.astype(I32)
    rank = jnp.concatenate([rank[:qd], rank[qd:]], axis=1)
    rank_ref[...] = rank
    ids = ids_ref[...]
    owner = ids // half
    offset = ids - owner * half
    local = rank - h * share
    place = owner * 256 + local
    inside = (local >= 0) & (local < share)
    a_ref[...] = jnp.where(inside, place // 128, -1)
    c_ref[...] = place % 128
    v0_ref[...] = (offset % 128).astype(F32)
    v1_ref[...] = (offset // 128).astype(F32)
    q_ref[...] = iota((qd, width), 0).astype(F32)
    na = 2 * nbeam
    arow = iota((na, width), 0)
    crow = iota((128, width), 0)

    def step(r, total):
        one = pl.ds(r, 1)
        hit = arow == a_ref[one, :]
        left = jnp.concatenate([jnp.where(hit, ref[one, :], 0.0) for ref in (v0_ref, v1_ref, q_ref)], axis=0)
        right = (crow == c_ref[one, :]).astype(F32)
        return total + lax.dot_general(left.astype(BF16), right.astype(BF16), NT, preferred_element_type=F32)

    table = lax.fori_loop(0, qd, step, jnp.zeros((3 * na, 128), F32), unroll=8).astype(I32)
    offs = table[:na] + 128 * table[na : 2 * na]
    qs = table[2 * na :]
    for o in range(nbeam):
        req_ref[o, 0:2, :] = offs[2 * o : 2 * o + 2]
        req_ref[o, 2:4, :] = qs[2 * o : 2 * o + 2]


def table_copies(table_ref, buf_ref, sems):
    groups = table_ref.shape[0] // 8
    width = table_ref.shape[1]
    src = table_ref.reshape(groups, 8, width)
    dst = buf_ref.reshape(groups, 4, 2, width)
    return [pltpu.make_async_copy(src.at[:, 2 * p : 2 * p + 2, :], dst.at[:, p], sems.at[p]) for p in range(4)]


def gather(share, off_ref, buf_ref, rows_ref, first, count):
    def one(b, _):
        for k in range(share):
            rows_ref[b * share + k] = buf_ref[off_ref[first + b, k // 128, k % 128]]
        return 0

    lax.fori_loop(0, count, one, 0)


def split2(x):
    hi = x.astype(BF16)
    return hi, (x - hi.astype(F32)).astype(BF16)


def score(share, b0, nb, qd, req_ref, rows_ref, queries_ref, wq_ref, wc_ref, wx_ref, vec_ref, out_ref):
    shards = wq_ref.shape[0]
    width = queries_ref.shape[1]
    m = nb * 2 * share
    qrows = []
    dup = (iota((2 * share, share), 0) // 2 == iota((2 * share, share), 1)).astype(BF16)
    for i in range(nb):
        b = b0 + i
        qvec = jnp.concatenate([req_ref[b, 2:3, :], req_ref[b, 3:4, : share - 128]], axis=1)
        oht = (iota((qd, share), 0) == qvec).astype(F32).astype(BF16)
        qb = queries_ref[pl.ds(pl.multiple_of(b * qd, qd), qd), :]
        qrow = lax.dot_general(oht, qb, TN, preferred_element_type=F32).astype(BF16)
        qrows.append(jnp.dot(dup, qrow, preferred_element_type=F32).astype(BF16))
    qrow = jnp.concatenate(qrows, axis=0) if nb > 1 else qrows[0]
    child = rows_ref[...].reshape(m, width)
    cross = child * qrow
    acc = jnp.zeros((m, 128), F32)
    for n in range(0, shards, 2):
        pair = lambda ref: jnp.concatenate([ref[n], ref[n + 1]], axis=1)
        pre = jnp.dot(child, pair(wc_ref), preferred_element_type=F32)
        pre += jnp.dot(cross, pair(wx_ref), preferred_element_type=F32)
        pre += jnp.dot(qrow, pair(wq_ref), preferred_element_type=F32)
        for j in range(2):
            part = pre[:, 128 * j : 128 * j + 128]
            acc += jnp.maximum(part + vec_ref[n + j, 0:1, :], 0.0) * vec_ref[n + j, 1:2, :]
    total = acc.T
    total = jnp.sum(total, axis=0, keepdims=True)
    for i in range(nb):
        for t in range(2 * share // 128):
            lo = i * 2 * share + t * 128
            out_ref[b0 + i, t : t + 1, :] = total[:, lo : lo + 128]


def unpermute(h, nhid, nbeam, share, half, ids_ref, rank_ref, sall_ref, out_ref):
    qd, width = ids_ref.shape
    per = width // nhid

    def own(x):
        mine = jnp.zeros((qd, per), I32)
        for k in range(nhid):
            mine = jnp.where(h == k, x[:, k * per : (k + 1) * per], mine)
        return jnp.concatenate([mine[8 * g : 8 * g + 8] for g in range(qd // 8)], axis=1)

    owner = own(ids_ref[...]) // half
    rank = own(rank_ref[...])
    chunk = rank // share
    local = rank - chunk * share
    tiles = 2 * share // 128
    row = (chunk * nbeam + owner) * tiles + local // 64
    lane = (local % 64) * 2
    nrows = nhid * nbeam * tiles
    scores = sall_ref[...].reshape(nrows, 128).T
    hi, lo = split2(scores)
    parts = jnp.concatenate([hi, lo], axis=0)
    lanes = lane.shape[1]
    rio = iota((nrows, lanes), 0)
    cio = iota((128, lanes), 0)
    evens, odds = [], []
    for i in range(8):
        onehot = (rio == row[i : i + 1]).astype(F32).astype(BF16)
        got = jnp.dot(parts, onehot, preferred_element_type=F32)
        got = got[:128] + got[128:]
        evens.append(jnp.sum(jnp.where(cio == lane[i : i + 1], got, 0.0), axis=0, keepdims=True))
        odds.append(jnp.sum(jnp.where(cio == lane[i : i + 1] + 1, got, 0.0), axis=0, keepdims=True))
    even = jnp.concatenate(split2(jnp.concatenate(evens, axis=0)), axis=0)
    odd = jnp.concatenate(split2(jnp.concatenate(odds, axis=0)), axis=0)
    n = iota((lanes, 2 * lanes), 1)
    k = iota((lanes, 2 * lanes), 0)
    mixed = jnp.dot(even, (n == 2 * k).astype(BF16), preferred_element_type=F32)
    mixed += jnp.dot(odd, (n == 2 * k + 1).astype(BF16), preferred_element_type=F32)
    mixed = mixed[:8] + mixed[8:]
    for g in range(qd // 8):
        out_ref[8 * g : 8 * g + 8, :] = mixed[:, 2 * per * g : 2 * per * (g + 1)]


BEAM, HID = 16, 8
MESH = pl.DeviceIdType.MESH
VM = pl.BlockSpec(memory_space=pltpu.VMEM)
ANY = pl.BlockSpec(memory_space=pltpu.HBM)


def shape(dims, dtype):
    return jax.ShapeDtypeStruct(dims, dtype)


def dma(*dims):
    return pltpu.SemaphoreType.DMA(dims)


def remote(src, dst, send, recv, device):
    return pltpu.make_async_remote_copy(
        src_ref=src, dst_ref=dst, send_sem=send, recv_sem=recv, device_id=device, device_id_type=MESH
    )


def loop(lo, hi, body):
    def step(i, _):
        body(i)
        return 0

    lax.fori_loop(lo, hi, step, 0)


def front_kernel(
    share,
    ids,
    queries,
    wq,
    wc,
    wx,
    bias,
    w_out,
    table,
    rank,
    req_all,
    q_all,
    w_all,
    vec_all,
    buf,
    req,
    a_ref,
    c_ref,
    v0_ref,
    v1_ref,
    qi_ref,
    table_sem,
    own_sem,
    rsend,
    rrecv,
    qsend,
    qrecv,
    vsend,
    vrecv,
    wsend,
    wrecv,
    psend,
    precv,
):
    b, h = lax.axis_index("beam"), lax.axis_index("hid")
    core = lax.rem(b, 2)
    mate = b + 1 - 2 * core
    z = lax.rem(h, 2)
    across = h + 1 - 2 * z
    qd = ids.shape[0]
    half = table.shape[0] // 2
    depth = w_all.shape[2] // 2

    def beam_peer(j):
        return lax.rem(b + j, BEAM)

    def hid_peer(j):
        return lax.rem(h + j, HID)

    def x_peer(j):
        return lax.rem(h + 2 * j, HID)

    barrier = pltpu.get_barrier_semaphore()
    loop(1, BEAM, lambda j: pl.semaphore_signal(barrier, inc=1, device_id=(beam_peer(j), h), device_id_type=MESH))
    loop(1, HID, lambda j: pl.semaphore_signal(barrier, inc=1, device_id=(b, hid_peer(j)), device_id_type=MESH))

    def q_rows(i):
        return pl.ds(pl.multiple_of(i * qd, qd), qd)

    own = [
        pltpu.make_async_copy(src, w_all.at[h, i], own_sem.at[i]) for i, src in enumerate((wq, wc, wx))
    ]
    own.append(pltpu.make_async_copy(queries, q_all.at[q_rows(b), :], own_sem.at[3]))
    own.append(pltpu.make_async_copy(bias, vec_all.at[h, 0:1, :], own_sem.at[4]))
    own.append(pltpu.make_async_copy(w_out, vec_all.at[h, 1:2, :], own_sem.at[5]))
    for copy in own:
        copy.start()
    pulls = table_copies(table, buf, table_sem)
    for copy in pulls:
        copy.start()
    for copy in own:
        copy.wait()
    pl.semaphore_wait(barrier, BEAM + HID - 2)

    def piece(shard, part):
        return w_all.at[shard, :, pl.ds(pl.multiple_of(part * depth, depth), depth), :]

    def w_copy(shard, to, slot):
        return remote(piece(shard, core), piece(shard, core), wsend.at[slot], wrecv.at[shard], (b, to))

    def mate_copy(shard):
        return remote(piece(shard, core), piece(shard, core), psend.at[shard], precv.at[shard], (mate, h))

    def mate_arrival(shard):
        other = piece(shard, 1 - core)
        return remote(other, other, psend.at[shard], precv.at[shard], (mate, h))

    def q_copy(to, slot):
        return remote(q_all.at[q_rows(slot), :], q_all.at[q_rows(slot), :], qsend.at[to], qrecv.at[slot], (to, h))

    def v_copy(to, slot):
        return remote(vec_all.at[slot], vec_all.at[slot], vsend.at[to], vrecv.at[slot], (b, to))

    def r_copy(to, slot):
        return remote(req.at[to], req_all.at[slot], rsend.at[to], rrecv.at[slot], (to, h))

    w_copy(h, across, 0).start()
    for j in range(1, 4):
        w_copy(h, x_peer(j), j).start()
    loop(1, HID, lambda j: v_copy(hid_peer(j), h).start())
    loop(1, BEAM, lambda j: q_copy(beam_peer(j), b).start())

    route(h, BEAM, share, half, ids, req, rank, a_ref, c_ref, v0_ref, v1_ref, qi_ref)
    loop(1, BEAM, lambda j: r_copy(beam_peer(j), b).start())
    req_all[pl.ds(b, 1)] = req[pl.ds(b, 1)]

    w_copy(across, across, 0).wait_recv()
    for j in range(1, 4):
        w_copy(across, x_peer(j), 3 + j).start()
    mate_copy(across).start()

    loop(1, BEAM, lambda j: r_copy(beam_peer(j), beam_peer(j)).wait_recv())
    for copy in pulls:
        copy.wait()

    for j in range(1, 4):
        for zz in (h, across):
            shard = lax.rem(zz + 2 * j, HID)
            w_copy(shard, shard, 0).wait_recv()
            mate_copy(shard).start()
    loop(1, BEAM, lambda j: q_copy(beam_peer(j), beam_peer(j)).wait_recv())
    loop(1, HID, lambda j: v_copy(hid_peer(j), hid_peer(j)).wait_recv())
    loop(1, HID, lambda j: mate_arrival(hid_peer(j)).wait_recv())

    w_copy(h, across, 0).wait_send()
    for j in range(1, 4):
        w_copy(h, x_peer(j), j).wait_send()
        w_copy(across, x_peer(j), 3 + j).wait_send()
    loop(1, BEAM, lambda j: q_copy(beam_peer(j), b).wait_send())
    loop(1, BEAM, lambda j: r_copy(beam_peer(j), b).wait_send())
    loop(1, HID, lambda j: v_copy(hid_peer(j), h).wait_send())
    loop(1, HID, lambda j: mate_copy(hid_peer(j)).wait_send())


def back_kernel(scores, sall, bsend, brecv, hsend, hrecv):
    b, h = lax.axis_index("beam"), lax.axis_index("hid")

    def beam_peer(j):
        return lax.rem(b + j, BEAM)

    def hid_peer(j):
        return lax.rem(h + j, HID)

    barrier = pltpu.get_barrier_semaphore()
    loop(1, BEAM, lambda j: pl.semaphore_signal(barrier, inc=1, device_id=(beam_peer(j), h), device_id_type=MESH))
    loop(1, HID, lambda j: pl.semaphore_signal(barrier, inc=1, device_id=(b, hid_peer(j)), device_id_type=MESH))
    pl.semaphore_wait(barrier, BEAM + HID - 2)

    def back(to, slot):
        return remote(scores.at[to], sall.at[h, slot], bsend.at[to], brecv.at[slot], (to, h))

    def spread(to, slot):
        return remote(sall.at[slot], sall.at[slot], hsend.at[to], hrecv.at[slot], (b, to))

    loop(1, BEAM, lambda j: back(beam_peer(j), b).start())
    sall[h, pl.ds(b, 1)] = scores[pl.ds(b, 1)]
    loop(1, BEAM, lambda j: back(beam_peer(j), beam_peer(j)).wait_recv())
    loop(1, HID, lambda j: spread(hid_peer(j), h).start())
    loop(1, BEAM, lambda j: back(beam_peer(j), b).wait_send())
    loop(1, HID, lambda j: spread(hid_peer(j), h).wait_send())
    loop(1, HID, lambda j: spread(hid_peer(j), hid_peer(j)).wait_recv())


def score_kernel(share, nb, qd, req, off, queries, w_all, vec, buf, scores, rows):
    def step(i):
        gather(share, off, buf, rows, i * nb, nb)
        score(share, i * nb, nb, qd, req, rows, queries, w_all.at[:, 0], w_all.at[:, 1], w_all.at[:, 2], vec, scores)

    loop(0, BEAM // nb, step)


def shards(queries, beam_ids, child_table, w_query, w_child, w_cross, bias, w_out):
    qd, width = beam_ids.shape
    embed = queries.shape[1]
    half = child_table.shape[0] // 2
    hid_dev = w_query.shape[1]
    share = 3 * qd * width // (2 * BEAM * HID)
    nb = 4
    ints = pltpu.VMEM((qd, width), I32)
    floats = pltpu.VMEM((qd, width), F32)

    rank, req_all, q_all, w_all, vec_all, buf = pl.pallas_call(
        functools.partial(front_kernel, share),
        out_shape=(
            shape((qd, width), I32),
            shape((BEAM, 4, 128), I32),
            pltpu.VMEM((BEAM * qd, embed), BF16),
            pltpu.VMEM((HID, 3, embed, hid_dev), BF16),
            pltpu.VMEM((HID, 2, hid_dev), F32),
            pltpu.VMEM((half, 2, embed), BF16),
        ),
        in_specs=[VM] + [ANY] * 7,
        out_specs=(VM,) * 6,
        scratch_shapes=[
            pltpu.VMEM((BEAM, 4, 128), I32),
            ints,
            ints,
            floats,
            floats,
            floats,
            dma(4),
            dma(6),
            *[dma(BEAM)] * 4,
            *[dma(HID)] * 2,
            dma(7),
            dma(HID),
            *[dma(HID)] * 2,
        ],
        compiler_params=pltpu.CompilerParams(collective_id=0, has_side_effects=True, vmem_limit_bytes=45 * 2**20),
        name="front",
    )(beam_ids, queries, w_query, w_child, w_cross, bias.reshape(1, -1), w_out.reshape(1, -1), child_table)

    scores = pl.pallas_call(
        functools.partial(score_kernel, share, nb, qd),
        out_shape=shape((BEAM, 3, 128), F32),
        in_specs=[VM, pl.BlockSpec(memory_space=pltpu.SMEM)] + [VM] * 4,
        out_specs=VM,
        scratch_shapes=[pltpu.VMEM((nb * share, 2, embed), BF16)],
        compiler_params=pltpu.CompilerParams(vmem_limit_bytes=20 * 2**20),
        name="score",
    )(req_all, req_all, q_all, w_all, vec_all, buf)

    sall = pl.pallas_call(
        back_kernel,
        out_shape=shape((HID, BEAM, 3, 128), F32),
        in_specs=[VM],
        out_specs=VM,
        scratch_shapes=[dma(BEAM), dma(BEAM), dma(HID), dma(HID)],
        compiler_params=pltpu.CompilerParams(collective_id=1, has_side_effects=True),
        name="give_back",
    )(scores)

    def place_kernel(ids, rank, sall, out):
        unpermute(lax.axis_index("hid"), HID, BEAM, share, half, ids, rank, sall, out)

    return pl.pallas_call(
        place_kernel,
        out_shape=shape((qd, 2 * width // HID), F32),
        in_specs=[VM] * 3,
        out_specs=VM,
        name="place",
    )(beam_ids, rank, sall)


def solution(mesh):
    return jax.shard_map(
        shards,
        mesh=mesh,
        in_specs=(
            P("beam", None),
            P("beam", None),
            P("beam", None),
            P(None, "hid"),
            P(None, "hid"),
            P(None, "hid"),
            P("hid"),
            P("hid"),
        ),
        out_specs=P("beam", "hid"),
        check_vma=False,
    )
```

```python
import functools
import math

import jax
import jax.numpy as jnp
from jax import lax
from jax.experimental import pallas as pl
from jax.experimental.pallas import tpu as pltpu
from jax.sharding import PartitionSpec as P

F32, BF16, I32 = jnp.float32, jnp.bfloat16, jnp.int32
NT = (((1,), (1,)), ((), ()))
TN = (((0,), (0,)), ((), ()))


def iota(shape, dim):
    return lax.broadcasted_iota(I32, shape, dim)


def route(h, nbeam, share, half, midway, ids_ref, req_ref, rank_ref, a_ref, c_ref, v0_ref, v1_ref, q_ref):
    qd, width = ids_ref.shape
    lo = ids_ref[:, :128]
    hi = ids_ref[:, 128:]
    ids = jnp.concatenate([lo, hi], axis=0)
    rows = ids.shape[0]
    owner = ids // half
    before_lane = (iota((128, 128), 0) < iota((128, 128), 1)).astype(BF16)
    ones = jnp.ones((128, 128), BF16)
    both = jnp.concatenate([before_lane, ones], axis=1)
    before_row = (iota((rows, rows), 1) < iota((rows, rows), 0)).astype(BF16)
    rank = jnp.zeros((rows, 128), F32)
    for o in range(nbeam):
        hit = owner == o
        counts = jnp.dot(hit.astype(BF16), both, preferred_element_type=F32)
        above = jnp.dot(before_row, counts[:, 128:].astype(BF16), preferred_element_type=F32)
        rank = rank + jnp.where(hit, counts[:, :128] + above, 0.0)
    rank = rank.astype(I32)
    rank = jnp.concatenate([rank[:qd], rank[qd:]], axis=1)
    rank_ref[...] = rank
    ids = ids_ref[...]
    owner = ids // half
    offset = ids - owner * half
    local = rank - h * share
    place = owner * 256 + local
    inside = (local >= 0) & (local < share)
    a_ref[...] = jnp.where(inside, place // 128, -1)
    c_ref[...] = place % 128
    v0_ref[...] = (offset % 128).astype(F32)
    v1_ref[...] = (offset // 128).astype(F32)
    q_ref[...] = iota((qd, width), 0).astype(F32)
    na = 2 * nbeam
    arow = iota((na, width), 0)
    crow = iota((128, width), 0)

    def step(r, total):
        one = pl.ds(r, 1)
        hit = arow == a_ref[one, :]
        left = jnp.concatenate([jnp.where(hit, ref[one, :], 0.0) for ref in (v0_ref, v1_ref, q_ref)], axis=0)
        right = (crow == c_ref[one, :]).astype(F32)
        return total + lax.dot_general(left.astype(BF16), right.astype(BF16), NT, preferred_element_type=F32)

    table = lax.fori_loop(0, qd // 2, step, jnp.zeros((3 * na, 128), F32), unroll=8)
    midway()
    table = lax.fori_loop(qd // 2, qd, step, table, unroll=8).astype(I32)
    offs = table[:na] + 128 * table[na : 2 * na]
    qs = table[2 * na :]
    for o in range(nbeam):
        req_ref[o, 0:2, :] = offs[2 * o : 2 * o + 2]
        req_ref[o, 2:4, :] = qs[2 * o : 2 * o + 2]


def table_copies(table_ref, buf_ref, sems):
    groups = table_ref.shape[0] // 8
    width = table_ref.shape[1]
    src = table_ref.reshape(groups, 8, width)
    dst = buf_ref.reshape(groups, 4, 2, width)
    return [pltpu.make_async_copy(src.at[:, 2 * p : 2 * p + 2, :], dst.at[:, p], sems.at[p]) for p in range(4)]


def gather(share, off_ref, buf_ref, rows_ref, first, count):
    def one(b, _):
        for k in range(share):
            rows_ref[b * share + k] = buf_ref[off_ref[first + b, k // 128, k % 128]]
        return 0

    lax.fori_loop(0, count, one, 0)


def split2(x):
    hi = x.astype(BF16)
    return hi, (x - hi.astype(F32)).astype(BF16)


def score(share, b0, nb, qd, twice_ref, rows_ref, queries_ref, wq_ref, wc_ref, wx_ref, vec_ref, out_ref):
    shards = wq_ref.shape[0]
    width = queries_ref.shape[1]
    m = nb * 2 * share
    qrows = []
    for i in range(nb):
        b = b0 + i
        oht = (iota((qd, 2 * share), 0) == twice_ref[pl.ds(b, 1), :]).astype(F32).astype(BF16)
        qb = queries_ref[pl.ds(pl.multiple_of(b * qd, qd), qd), :]
        qrows.append(lax.dot_general(oht, qb, TN, preferred_element_type=F32).astype(BF16))
    qrow = jnp.concatenate(qrows, axis=0) if nb > 1 else qrows[0]
    child = rows_ref[...].reshape(m, width)
    cross = child * qrow
    acc = jnp.zeros((m, 128), F32)
    for n in range(0, shards, 2):
        pair = lambda ref: jnp.concatenate([ref[n], ref[n + 1]], axis=1)
        pre = jnp.dot(child, pair(wc_ref), preferred_element_type=F32)
        pre += jnp.dot(cross, pair(wx_ref), preferred_element_type=F32)
        pre += jnp.dot(qrow, pair(wq_ref), preferred_element_type=F32)
        for j in range(2):
            part = pre[:, 128 * j : 128 * j + 128]
            acc += jnp.maximum(part + vec_ref[n + j, 0:1, :], 0.0) * vec_ref[n + j, 1:2, :]
    total = acc.T
    total = jnp.sum(total, axis=0, keepdims=True)
    for i in range(nb):
        for t in range(2 * share // 128):
            lo = i * 2 * share + t * 128
            out_ref[b0 + i, t : t + 1, :] = total[:, lo : lo + 128]


def unpermute(h, nhid, nbeam, share, half, ids_ref, rank_ref, sall_ref, out_ref):
    qd, width = ids_ref.shape
    per = width // nhid

    def own(x):
        mine = jnp.zeros((qd, per), I32)
        for k in range(nhid):
            mine = jnp.where(h == k, x[:, k * per : (k + 1) * per], mine)
        return jnp.concatenate([mine[8 * g : 8 * g + 8] for g in range(qd // 8)], axis=1)

    owner = own(ids_ref[...]) // half
    rank = own(rank_ref[...])
    chunk = rank // share
    local = rank - chunk * share
    tiles = 2 * share // 128
    row = (chunk * nbeam + owner) * tiles + local // 64
    lane = (local % 64) * 2
    nrows = nhid * nbeam * tiles
    scores = sall_ref[...].reshape(nrows, 128).T
    hi, lo = split2(scores)
    parts = jnp.concatenate([hi, lo], axis=0)
    lanes = lane.shape[1]
    rio = iota((nrows, lanes), 0)
    cio = iota((128, lanes), 0)
    evens, odds = [], []
    for i in range(8):
        onehot = (rio == row[i : i + 1]).astype(F32).astype(BF16)
        got = jnp.dot(parts, onehot, preferred_element_type=F32)
        got = got[:128] + got[128:]
        evens.append(jnp.sum(jnp.where(cio == lane[i : i + 1], got, 0.0), axis=0, keepdims=True))
        odds.append(jnp.sum(jnp.where(cio == lane[i : i + 1] + 1, got, 0.0), axis=0, keepdims=True))
    even = jnp.concatenate(split2(jnp.concatenate(evens, axis=0)), axis=0)
    odd = jnp.concatenate(split2(jnp.concatenate(odds, axis=0)), axis=0)
    n = iota((lanes, 2 * lanes), 1)
    k = iota((lanes, 2 * lanes), 0)
    mixed = jnp.dot(even, (n == 2 * k).astype(BF16), preferred_element_type=F32)
    mixed += jnp.dot(odd, (n == 2 * k + 1).astype(BF16), preferred_element_type=F32)
    mixed = mixed[:8] + mixed[8:]
    for g in range(qd // 8):
        out_ref[8 * g : 8 * g + 8, :] = mixed[:, 2 * per * g : 2 * per * (g + 1)]


BEAM, HID = 16, 8
MESH = pl.DeviceIdType.MESH
VM = pl.BlockSpec(memory_space=pltpu.VMEM)
ANY = pl.BlockSpec(memory_space=pltpu.HBM)


def shape(dims, dtype):
    return jax.ShapeDtypeStruct(dims, dtype)


def dma(*dims):
    return pltpu.SemaphoreType.DMA(dims)


def remote(src, dst, send, recv, device):
    return pltpu.make_async_remote_copy(
        src_ref=src, dst_ref=dst, send_sem=send, recv_sem=recv, device_id=device, device_id_type=MESH
    )


def loop(lo, hi, body):
    def step(i, _):
        body(i)
        return 0

    lax.fori_loop(lo, hi, step, 0)


def front_kernel(
    share,
    ids,
    queries,
    wq,
    wc,
    wx,
    bias,
    w_out,
    table,
    rank,
    req_all,
    q_all,
    w_all,
    vec_all,
    buf,
    req,
    a_ref,
    c_ref,
    v0_ref,
    v1_ref,
    qi_ref,
    table_sem,
    own_sem,
    rsend,
    rrecv,
    qsend,
    qrecv,
    vsend,
    vrecv,
    wsend,
    wrecv,
    psend,
    precv,
    fsend,
    frecv,
):
    b, h = lax.axis_index("beam"), lax.axis_index("hid")
    core = lax.rem(b, 2)
    mate = b + 1 - 2 * core
    z = lax.rem(h, 2)
    across = h + 1 - 2 * z
    beyond = lax.rem(b + BEAM // 2, BEAM)
    qd = ids.shape[0]
    half = table.shape[0] // 2
    depth = w_all.shape[2] // 2

    def beam_peer(j):
        return lax.rem(b + j, BEAM)

    def hid_peer(j):
        return lax.rem(h + j, HID)

    def x_peer(j):
        return lax.rem(h + 2 * j, HID)

    barrier = pltpu.get_barrier_semaphore()
    loop(1, BEAM, lambda j: pl.semaphore_signal(barrier, inc=1, device_id=(beam_peer(j), h), device_id_type=MESH))
    loop(1, HID, lambda j: pl.semaphore_signal(barrier, inc=1, device_id=(b, hid_peer(j)), device_id_type=MESH))
    pl.semaphore_signal(barrier, inc=1, device_id=(beyond, across), device_id_type=MESH)

    def q_rows(i):
        return pl.ds(pl.multiple_of(i * qd, qd), qd)

    own = [
        pltpu.make_async_copy(src, w_all.at[h, i], own_sem.at[i]) for i, src in enumerate((wq, wc, wx))
    ]
    own.append(pltpu.make_async_copy(queries, q_all.at[q_rows(b), :], own_sem.at[3]))
    own.append(pltpu.make_async_copy(bias, vec_all.at[h, 0:1, :], own_sem.at[4]))
    own.append(pltpu.make_async_copy(w_out, vec_all.at[h, 1:2, :], own_sem.at[5]))
    for copy in own:
        copy.start()
    pulls = table_copies(table, buf, table_sem)
    for copy in pulls:
        copy.start()
    for copy in own:
        copy.wait()
    pl.semaphore_wait(barrier, BEAM + HID - 1)

    def piece(shard, part):
        return w_all.at[shard, :, pl.ds(pl.multiple_of(part * depth, depth), depth), :]

    def w_copy(shard, to, slot):
        return remote(piece(shard, core), piece(shard, core), wsend.at[slot], wrecv.at[shard], (b, to))

    def z_copy(shard):
        return remote(piece(shard, core), piece(shard, core), wsend.at[0], wrecv.at[shard], (beyond, across))

    def quarter(shard, side):
        start = pl.multiple_of(core * depth + side * (depth // 2), depth // 2)
        return w_all.at[shard, :, pl.ds(start, depth // 2), :]

    def pass_on(shard, side, to):
        return remote(quarter(shard, side), quarter(shard, side), fsend.at[side], frecv.at[side], (b, to))

    def mate_copy(shard):
        return remote(piece(shard, core), piece(shard, core), psend.at[shard], precv.at[shard], (mate, h))

    def mate_arrival(shard):
        other = piece(shard, 1 - core)
        return remote(other, other, psend.at[shard], precv.at[shard], (mate, h))

    def q_copy(to, slot):
        return remote(q_all.at[q_rows(slot), :], q_all.at[q_rows(slot), :], qsend.at[to], qrecv.at[slot], (to, h))

    def v_copy(to, slot):
        return remote(vec_all.at[slot], vec_all.at[slot], vsend.at[to], vrecv.at[slot], (b, to))

    def r_copy(to, slot):
        return remote(req.at[to], req_all.at[slot], rsend.at[to], rrecv.at[slot], (to, h))

    z_copy(h).start()
    for j in range(1, 4):
        w_copy(h, x_peer(j), j).start()
    loop(1, HID, lambda j: v_copy(hid_peer(j), h).start())
    loop(1, BEAM, lambda j: q_copy(beam_peer(j), b).start())

    def midway():
        z_copy(across).wait_recv()
        for j in (1, 3):
            w_copy(across, x_peer(j), 3 + j).start()
        mate_copy(across).start()

    route(h, BEAM, share, half, midway, ids, req, rank, a_ref, c_ref, v0_ref, v1_ref, qi_ref)
    loop(1, BEAM, lambda j: r_copy(beam_peer(j), b).start())
    req_all[pl.ds(b, 1)] = req[pl.ds(b, 1)]


    near = [lax.rem(across + 2 * j, HID) for j in (1, 3)]
    far = lax.rem(across + 4, HID)
    for j in (1, 3):
        w_copy(x_peer(j), x_peer(j), 0).wait_recv()
        mate_copy(x_peer(j)).start()
    for side, shard in enumerate(near):
        w_copy(shard, shard, 0).wait_recv()
        pass_on(shard, side, x_peer(3 - 2 * side)).start()
        mate_copy(shard).start()
    w_copy(x_peer(2), x_peer(2), 0).wait_recv()
    mate_copy(x_peer(2)).start()
    for side in range(2):
        pass_on(far, side, x_peer(3 - 2 * side)).wait_recv()
    mate_copy(far).start()
    loop(1, BEAM, lambda j: r_copy(beam_peer(j), beam_peer(j)).wait_recv())
    for copy in pulls:
        copy.wait()
    loop(1, BEAM, lambda j: q_copy(beam_peer(j), beam_peer(j)).wait_recv())
    loop(1, HID, lambda j: v_copy(hid_peer(j), hid_peer(j)).wait_recv())
    loop(1, HID, lambda j: mate_arrival(hid_peer(j)).wait_recv())

    z_copy(h).wait_send()
    for j in range(1, 4):
        w_copy(h, x_peer(j), j).wait_send()
    for j in (1, 3):
        w_copy(across, x_peer(j), 3 + j).wait_send()
    for side, shard in enumerate(near):
        pass_on(shard, side, x_peer(3 - 2 * side)).wait_send()
    loop(1, BEAM, lambda j: q_copy(beam_peer(j), b).wait_send())
    loop(1, BEAM, lambda j: r_copy(beam_peer(j), b).wait_send())
    loop(1, HID, lambda j: v_copy(hid_peer(j), h).wait_send())
    loop(1, HID, lambda j: mate_copy(hid_peer(j)).wait_send())


def back_kernel(scores, sall, bsend, brecv, hsend, hrecv):
    b, h = lax.axis_index("beam"), lax.axis_index("hid")

    def beam_peer(j):
        return lax.rem(b + j, BEAM)

    def hid_peer(j):
        return lax.rem(h + j, HID)

    barrier = pltpu.get_barrier_semaphore()
    loop(1, BEAM, lambda j: pl.semaphore_signal(barrier, inc=1, device_id=(beam_peer(j), h), device_id_type=MESH))
    loop(1, HID, lambda j: pl.semaphore_signal(barrier, inc=1, device_id=(b, hid_peer(j)), device_id_type=MESH))
    pl.semaphore_wait(barrier, BEAM + HID - 2)

    def back(to, slot):
        return remote(scores.at[to], sall.at[h, slot], bsend.at[to], brecv.at[slot], (to, h))

    def spread(to, slot):
        return remote(sall.at[slot], sall.at[slot], hsend.at[to], hrecv.at[slot], (b, to))

    loop(1, BEAM, lambda j: back(beam_peer(j), b).start())
    sall[h, pl.ds(b, 1)] = scores[pl.ds(b, 1)]
    loop(1, BEAM, lambda j: back(beam_peer(j), beam_peer(j)).wait_recv())
    loop(1, HID, lambda j: spread(hid_peer(j), h).start())
    loop(1, BEAM, lambda j: back(beam_peer(j), b).wait_send())
    loop(1, HID, lambda j: spread(hid_peer(j), h).wait_send())
    loop(1, HID, lambda j: spread(hid_peer(j), hid_peer(j)).wait_recv())


def score_kernel(share, nb, qd, req, off, queries, w_all, vec, buf, scores, rows, twice):
    lists = req[...]
    qs = jnp.concatenate([lists[:, 2, :], lists[:, 3, : share - 128]], axis=1).astype(F32).astype(BF16)
    dup = (iota((share, 2 * share), 1) // 2 == iota((share, 2 * share), 0)).astype(F32).astype(BF16)
    twice[...] = jnp.dot(qs, dup, preferred_element_type=F32).astype(I32)

    def step(i):
        gather(share, off, buf, rows, i * nb, nb)
        score(share, i * nb, nb, qd, twice, rows, queries, w_all.at[:, 0], w_all.at[:, 1], w_all.at[:, 2], vec, scores)

    loop(0, BEAM // nb, step)


def shards(queries, beam_ids, child_table, w_query, w_child, w_cross, bias, w_out):
    qd, width = beam_ids.shape
    embed = queries.shape[1]
    half = child_table.shape[0] // 2
    hid_dev = w_query.shape[1]
    share = 3 * qd * width // (2 * BEAM * HID)
    nb = 4
    ints = pltpu.VMEM((qd, width), I32)
    floats = pltpu.VMEM((qd, width), F32)

    rank, req_all, q_all, w_all, vec_all, buf = pl.pallas_call(
        functools.partial(front_kernel, share),
        out_shape=(
            shape((qd, width), I32),
            pltpu.VMEM((BEAM, 4, 128), I32),
            pltpu.VMEM((BEAM * qd, embed), BF16),
            pltpu.VMEM((HID, 3, embed, hid_dev), BF16),
            pltpu.VMEM((HID, 2, hid_dev), F32),
            pltpu.VMEM((half, 2, embed), BF16),
        ),
        in_specs=[VM] + [ANY] * 7,
        out_specs=(VM,) * 6,
        scratch_shapes=[
            pltpu.VMEM((BEAM, 4, 128), I32),
            ints,
            ints,
            floats,
            floats,
            floats,
            dma(4),
            dma(6),
            *[dma(BEAM)] * 4,
            *[dma(HID)] * 2,
            dma(7),
            dma(HID),
            *[dma(HID)] * 2,
            *[dma(2)] * 2,
        ],
        compiler_params=pltpu.CompilerParams(collective_id=0, has_side_effects=True, vmem_limit_bytes=45 * 2**20),
        name="front",
    )(beam_ids, queries, w_query, w_child, w_cross, bias.reshape(1, -1), w_out.reshape(1, -1), child_table)

    scores = pl.pallas_call(
        functools.partial(score_kernel, share, nb, qd),
        out_shape=pltpu.VMEM((BEAM, 3, 128), F32),
        in_specs=[VM, pl.BlockSpec(memory_space=pltpu.SMEM)] + [VM] * 4,
        out_specs=VM,
        scratch_shapes=[pltpu.VMEM((nb * share, 2, embed), BF16), pltpu.VMEM((BEAM, 2 * share), I32)],
        compiler_params=pltpu.CompilerParams(vmem_limit_bytes=20 * 2**20),
        name="score",
    )(req_all, req_all, q_all, w_all, vec_all, buf)

    sall = pl.pallas_call(
        back_kernel,
        out_shape=pltpu.VMEM((HID, BEAM, 3, 128), F32),
        in_specs=[VM],
        out_specs=VM,
        scratch_shapes=[dma(BEAM), dma(BEAM), dma(HID), dma(HID)],
        compiler_params=pltpu.CompilerParams(collective_id=1, has_side_effects=True, vmem_limit_bytes=8 * 2**20),
        name="give_back",
    )(scores)

    def place_kernel(ids, rank, sall, out):
        unpermute(lax.axis_index("hid"), HID, BEAM, share, half, ids, rank, sall, out)

    return pl.pallas_call(
        place_kernel,
        out_shape=shape((qd, 2 * width // HID), F32),
        in_specs=[VM] * 3,
        out_specs=VM,
        compiler_params=pltpu.CompilerParams(vmem_limit_bytes=56 * 2**20),
        name="place",
    )(beam_ids, rank, sall)


def solution(mesh):
    return jax.shard_map(
        shards,
        mesh=mesh,
        in_specs=(
            P("beam", None),
            P("beam", None),
            P("beam", None),
            P(None, "hid"),
            P(None, "hid"),
            P(None, "hid"),
            P("hid"),
            P("hid"),
        ),
        out_specs=P("beam", "hid"),
        check_vma=False,
    )
```

```python
import functools
import math

import jax
import jax.numpy as jnp
from jax import lax
from jax.experimental import pallas as pl
from jax.experimental.pallas import tpu as pltpu
from jax.sharding import PartitionSpec as P

F32, BF16, I32 = jnp.float32, jnp.bfloat16, jnp.int32
NT = (((1,), (1,)), ((), ()))
TN = (((0,), (0,)), ((), ()))


def iota(shape, dim):
    return lax.broadcasted_iota(I32, shape, dim)


def route(h, nbeam, share, half, midway, ids_ref, req_ref, rank_ref, a_ref, c_ref, v0_ref, v1_ref, q_ref):
    qd, width = ids_ref.shape
    lo = ids_ref[:, :128]
    hi = ids_ref[:, 128:]
    ids = jnp.concatenate([lo, hi], axis=0)
    rows = ids.shape[0]
    owner = ids // half
    before_lane = (iota((128, 128), 0) < iota((128, 128), 1)).astype(BF16)
    ones = jnp.ones((128, 128), BF16)
    both = jnp.concatenate([before_lane, ones], axis=1)
    before_row = (iota((rows, rows), 1) < iota((rows, rows), 0)).astype(BF16)
    rank = jnp.zeros((rows, 128), F32)
    for o in range(nbeam):
        hit = owner == o
        counts = jnp.dot(hit.astype(BF16), both, preferred_element_type=F32)
        above = jnp.dot(before_row, counts[:, 128:].astype(BF16), preferred_element_type=F32)
        rank = rank + jnp.where(hit, counts[:, :128] + above, 0.0)
    rank = rank.astype(I32)
    rank = jnp.concatenate([rank[:qd], rank[qd:]], axis=1)
    rank_ref[...] = rank
    ids = ids_ref[...]
    owner = ids // half
    offset = ids - owner * half
    local = rank - h * share
    place = owner * 256 + local
    inside = (local >= 0) & (local < share)
    a_ref[...] = jnp.where(inside, place // 128, -1)
    c_ref[...] = place % 128
    v0_ref[...] = (offset % 128).astype(F32)
    v1_ref[...] = (offset // 128).astype(F32)
    q_ref[...] = iota((qd, width), 0).astype(F32)
    na = 2 * nbeam
    arow = iota((na, width), 0)
    crow = iota((128, width), 0)

    def step(r, total):
        one = pl.ds(r, 1)
        hit = arow == a_ref[one, :]
        left = jnp.concatenate([jnp.where(hit, ref[one, :], 0.0) for ref in (v0_ref, v1_ref, q_ref)], axis=0)
        right = (crow == c_ref[one, :]).astype(F32)
        return total + lax.dot_general(left.astype(BF16), right.astype(BF16), NT, preferred_element_type=F32)

    table = lax.fori_loop(0, qd // 2, step, jnp.zeros((3 * na, 128), F32), unroll=8)
    midway()
    table = lax.fori_loop(qd // 2, qd, step, table, unroll=8).astype(I32)
    offs = table[:na] + 128 * table[na : 2 * na]
    qs = table[2 * na :]
    for o in range(nbeam):
        req_ref[o, 0:2, :] = offs[2 * o : 2 * o + 2]
        req_ref[o, 2:4, :] = qs[2 * o : 2 * o + 2]


def table_copies(table_ref, buf_ref, sems):
    groups = table_ref.shape[0] // 8
    width = table_ref.shape[1]
    src = table_ref.reshape(groups, 8, width)
    dst = buf_ref.reshape(groups, 4, 2, width)
    return [pltpu.make_async_copy(src.at[:, 2 * p : 2 * p + 2, :], dst.at[:, p], sems.at[p]) for p in range(4)]


def gather(share, off_ref, buf_ref, rows_ref, first, count):
    for i in range(count):
        for k in range(share):
            rows_ref[i * share + k] = buf_ref[off_ref[first + i, k // 128, k % 128]]


def split2(x):
    hi = x.astype(BF16)
    return hi, (x - hi.astype(F32)).astype(BF16)


def score(share, b0, nb, qd, twice_ref, rows_ref, queries_ref, wq_ref, wc_ref, wx_ref, vec_ref, out_ref):
    shards = wq_ref.shape[0]
    width = queries_ref.shape[1]
    m = nb * 2 * share
    qrows = []
    for i in range(nb):
        b = b0 + i
        oht = (iota((qd, 2 * share), 0) == twice_ref[pl.ds(b, 1), :]).astype(F32).astype(BF16)
        qb = queries_ref[pl.ds(pl.multiple_of(b * qd, qd), qd), :]
        qrows.append(lax.dot_general(oht, qb, TN, preferred_element_type=F32).astype(BF16))
    qrow = jnp.concatenate(qrows, axis=0) if nb > 1 else qrows[0]
    child = rows_ref[...].reshape(m, width)
    cross = child * qrow
    acc = jnp.zeros((m, 128), F32)
    for n in range(0, shards, 2):
        pair = lambda ref: jnp.concatenate([ref[n], ref[n + 1]], axis=1)
        pre = jnp.dot(child, pair(wc_ref), preferred_element_type=F32)
        pre += jnp.dot(cross, pair(wx_ref), preferred_element_type=F32)
        pre += jnp.dot(qrow, pair(wq_ref), preferred_element_type=F32)
        for j in range(2):
            part = pre[:, 128 * j : 128 * j + 128]
            acc += jnp.maximum(part + vec_ref[n + j, 0:1, :], 0.0) * vec_ref[n + j, 1:2, :]
    total = acc.T
    total = jnp.sum(total, axis=0, keepdims=True)
    for i in range(nb):
        for t in range(2 * share // 128):
            lo = i * 2 * share + t * 128
            out_ref[b0 + i, t : t + 1, :] = total[:, lo : lo + 128]


def unpermute(h, nhid, nbeam, share, half, ids_ref, rank_ref, sall_ref, out_ref):
    qd, width = ids_ref.shape
    per = width // nhid

    def own(x):
        mine = jnp.zeros((qd, per), I32)
        for k in range(nhid):
            mine = jnp.where(h == k, x[:, k * per : (k + 1) * per], mine)
        return jnp.concatenate([mine[8 * g : 8 * g + 8] for g in range(qd // 8)], axis=1)

    owner = own(ids_ref[...]) // half
    rank = own(rank_ref[...])
    chunk = rank // share
    local = rank - chunk * share
    tiles = 2 * share // 128
    row = (chunk * nbeam + owner) * tiles + local // 64
    lane = (local % 64) * 2
    nrows = nhid * nbeam * tiles
    scores = sall_ref[...].reshape(nrows, 128).T
    hi, lo = split2(scores)
    parts = jnp.concatenate([hi, lo], axis=0)
    lanes = lane.shape[1]
    rio = iota((nrows, lanes), 0)
    cio = iota((128, lanes), 0)
    evens, odds = [], []
    for i in range(8):
        onehot = (rio == row[i : i + 1]).astype(F32).astype(BF16)
        got = jnp.dot(parts, onehot, preferred_element_type=F32)
        got = got[:128] + got[128:]
        evens.append(jnp.sum(jnp.where(cio == lane[i : i + 1], got, 0.0), axis=0, keepdims=True))
        odds.append(jnp.sum(jnp.where(cio == lane[i : i + 1] + 1, got, 0.0), axis=0, keepdims=True))
    even = jnp.concatenate(split2(jnp.concatenate(evens, axis=0)), axis=0)
    odd = jnp.concatenate(split2(jnp.concatenate(odds, axis=0)), axis=0)
    n = iota((lanes, 2 * lanes), 1)
    k = iota((lanes, 2 * lanes), 0)
    mixed = jnp.dot(even, (n == 2 * k).astype(BF16), preferred_element_type=F32)
    mixed += jnp.dot(odd, (n == 2 * k + 1).astype(BF16), preferred_element_type=F32)
    mixed = mixed[:8] + mixed[8:]
    for g in range(qd // 8):
        out_ref[8 * g : 8 * g + 8, :] = mixed[:, 2 * per * g : 2 * per * (g + 1)]


BEAM, HID = 16, 8
MESH = pl.DeviceIdType.MESH
VM = pl.BlockSpec(memory_space=pltpu.VMEM)
ANY = pl.BlockSpec(memory_space=pltpu.HBM)


def shape(dims, dtype):
    return jax.ShapeDtypeStruct(dims, dtype)


def dma(*dims):
    return pltpu.SemaphoreType.DMA(dims)


def remote(src, dst, send, recv, device):
    return pltpu.make_async_remote_copy(
        src_ref=src, dst_ref=dst, send_sem=send, recv_sem=recv, device_id=device, device_id_type=MESH
    )


def loop(lo, hi, body):
    def step(i, _):
        body(i)
        return 0

    lax.fori_loop(lo, hi, step, 0)


def front_kernel(
    share,
    ids,
    queries,
    wq,
    wc,
    wx,
    bias,
    w_out,
    table,
    rank,
    req_all,
    q_all,
    w_all,
    vec_all,
    buf,
    req,
    a_ref,
    c_ref,
    v0_ref,
    v1_ref,
    qi_ref,
    table_sem,
    own_sem,
    rsend,
    rrecv,
    qsend,
    qrecv,
    vsend,
    vrecv,
    wsend,
    wrecv,
    psend,
    precv,
    fsend,
    frecv,
):
    b, h = lax.axis_index("beam"), lax.axis_index("hid")
    core = lax.rem(b, 2)
    mate = b + 1 - 2 * core
    z = lax.rem(h, 2)
    across = h + 1 - 2 * z
    beyond = lax.rem(b + BEAM // 2, BEAM)
    qd = ids.shape[0]
    half = table.shape[0] // 2
    depth = w_all.shape[2] // 2

    def beam_peer(j):
        return lax.rem(b + j, BEAM)

    def hid_peer(j):
        return lax.rem(h + j, HID)

    def x_peer(j):
        return lax.rem(h + 2 * j, HID)

    barrier = pltpu.get_barrier_semaphore()
    loop(1, BEAM, lambda j: pl.semaphore_signal(barrier, inc=1, device_id=(beam_peer(j), h), device_id_type=MESH))
    loop(1, HID, lambda j: pl.semaphore_signal(barrier, inc=1, device_id=(b, hid_peer(j)), device_id_type=MESH))
    pl.semaphore_signal(barrier, inc=1, device_id=(beyond, across), device_id_type=MESH)

    def q_rows(i):
        return pl.ds(pl.multiple_of(i * qd, qd), qd)

    own = [
        pltpu.make_async_copy(src, w_all.at[h, i], own_sem.at[i]) for i, src in enumerate((wq, wc, wx))
    ]
    own.append(pltpu.make_async_copy(queries, q_all.at[q_rows(b), :], own_sem.at[3]))
    own.append(pltpu.make_async_copy(bias, vec_all.at[h, 0:1, :], own_sem.at[4]))
    own.append(pltpu.make_async_copy(w_out, vec_all.at[h, 1:2, :], own_sem.at[5]))
    for copy in own:
        copy.start()
    pulls = table_copies(table, buf, table_sem)
    for copy in pulls:
        copy.start()
    for copy in own:
        copy.wait()
    pl.semaphore_wait(barrier, BEAM + HID - 1)

    def piece(shard, part):
        return w_all.at[shard, :, pl.ds(pl.multiple_of(part * depth, depth), depth), :]

    def w_copy(shard, to, slot):
        return remote(piece(shard, core), piece(shard, core), wsend.at[slot], wrecv.at[shard], (b, to))

    def z_copy(shard):
        return remote(piece(shard, core), piece(shard, core), wsend.at[0], wrecv.at[shard], (beyond, across))

    def quarter(shard, side):
        start = pl.multiple_of(core * depth + side * (depth // 2), depth // 2)
        return w_all.at[shard, :, pl.ds(start, depth // 2), :]

    def pass_on(shard, side, lane):
        part = quarter(shard, side)
        return remote(part, part, fsend.at[lane + side], frecv.at[lane + side], (b, x_peer(3 - 2 * side)))

    beside = [x_peer(j) for j in (1, 3)]
    near = [lax.rem(across + 2 * j, HID) for j in (1, 3)]
    ends = (x_peer(2), lax.rem(across + 4, HID))

    def mate_copy(shard):
        return remote(piece(shard, core), piece(shard, core), psend.at[shard], precv.at[shard], (mate, h))

    def mate_arrival(shard):
        other = piece(shard, 1 - core)
        return remote(other, other, psend.at[shard], precv.at[shard], (mate, h))

    def q_copy(to, slot):
        return remote(q_all.at[q_rows(slot), :], q_all.at[q_rows(slot), :], qsend.at[to], qrecv.at[slot], (to, h))

    def v_copy(to, slot):
        return remote(vec_all.at[slot], vec_all.at[slot], vsend.at[to], vrecv.at[slot], (b, to))

    def r_copy(to, slot):
        return remote(req.at[to], req_all.at[slot], rsend.at[to], rrecv.at[slot], (to, h))

    z_copy(h).start()
    for j in (1, 3):
        w_copy(h, x_peer(j), j).start()
    loop(1, HID, lambda j: v_copy(hid_peer(j), h).start())
    loop(1, BEAM, lambda j: q_copy(beam_peer(j), b).start())

    def midway():
        z_copy(across).wait_recv()
        for j in (1, 3):
            w_copy(across, x_peer(j), 3 + j).start()
        for side, shard in enumerate(beside):
            w_copy(shard, shard, 0).wait_recv()
            pass_on(shard, side, 0).start()
        mate_copy(across).start()
        for shard in beside:
            mate_copy(shard).start()

    route(h, BEAM, share, half, midway, ids, req, rank, a_ref, c_ref, v0_ref, v1_ref, qi_ref)
    loop(1, BEAM, lambda j: r_copy(beam_peer(j), b).start())
    req_all[pl.ds(b, 1)] = req[pl.ds(b, 1)]


    for side, shard in enumerate(near):
        w_copy(shard, shard, 0).wait_recv()
        pass_on(shard, side, 2).start()
        mate_copy(shard).start()
    for i, shard in enumerate(ends):
        for side in range(2):
            pass_on(shard, side, 2 * i).wait_recv()
        mate_copy(shard).start()
    loop(1, BEAM, lambda j: r_copy(beam_peer(j), beam_peer(j)).wait_recv())
    for copy in pulls:
        copy.wait()
    loop(1, BEAM, lambda j: q_copy(beam_peer(j), beam_peer(j)).wait_recv())
    loop(1, HID, lambda j: v_copy(hid_peer(j), hid_peer(j)).wait_recv())
    loop(1, HID, lambda j: mate_arrival(hid_peer(j)).wait_recv())

    z_copy(h).wait_send()
    for j in (1, 3):
        w_copy(h, x_peer(j), j).wait_send()
        w_copy(across, x_peer(j), 3 + j).wait_send()
    for i, pair in enumerate((beside, near)):
        for side, shard in enumerate(pair):
            pass_on(shard, side, 2 * i).wait_send()
    loop(1, BEAM, lambda j: q_copy(beam_peer(j), b).wait_send())
    loop(1, BEAM, lambda j: r_copy(beam_peer(j), b).wait_send())
    loop(1, HID, lambda j: v_copy(hid_peer(j), h).wait_send())
    loop(1, HID, lambda j: mate_copy(hid_peer(j)).wait_send())


def back_kernel(scores, sall, bsend, brecv, hsend, hrecv):
    b, h = lax.axis_index("beam"), lax.axis_index("hid")

    def beam_peer(j):
        return lax.rem(b + j, BEAM)

    def hid_peer(j):
        return lax.rem(h + j, HID)

    barrier = pltpu.get_barrier_semaphore()
    loop(1, BEAM, lambda j: pl.semaphore_signal(barrier, inc=1, device_id=(beam_peer(j), h), device_id_type=MESH))
    loop(1, HID, lambda j: pl.semaphore_signal(barrier, inc=1, device_id=(b, hid_peer(j)), device_id_type=MESH))
    pl.semaphore_wait(barrier, BEAM + HID - 2)

    def back(to, slot):
        return remote(scores.at[to], sall.at[h, slot], bsend.at[to], brecv.at[slot], (to, h))

    def spread(to, slot):
        return remote(sall.at[slot], sall.at[slot], hsend.at[to], hrecv.at[slot], (b, to))

    loop(1, BEAM, lambda j: back(beam_peer(j), b).start())
    sall[h, pl.ds(b, 1)] = scores[pl.ds(b, 1)]
    loop(1, BEAM, lambda j: back(beam_peer(j), beam_peer(j)).wait_recv())
    loop(1, HID, lambda j: spread(hid_peer(j), h).start())
    loop(1, BEAM, lambda j: back(beam_peer(j), b).wait_send())
    loop(1, HID, lambda j: spread(hid_peer(j), h).wait_send())
    loop(1, HID, lambda j: spread(hid_peer(j), hid_peer(j)).wait_recv())


def score_kernel(share, nb, qd, req, off, queries, w_all, vec, buf, scores, rows, rows2, twice):
    lists = req[...]
    qs = jnp.concatenate([lists[:, 2, :], lists[:, 3, : share - 128]], axis=1).astype(F32).astype(BF16)
    dup = (iota((share, 2 * share), 1) // 2 == iota((share, 2 * share), 0)).astype(F32).astype(BF16)
    twice[...] = jnp.dot(qs, dup, preferred_element_type=F32).astype(I32)

    def run(first, now, then):
        gather(share, off, buf, then, jnp.minimum(first + nb, BEAM - nb), nb)
        score(share, first, nb, qd, twice, now, queries, w_all.at[:, 0], w_all.at[:, 1], w_all.at[:, 2], vec, scores)

    def step(i):
        run(2 * i * nb, rows, rows2)
        run((2 * i + 1) * nb, rows2, rows)

    gather(share, off, buf, rows, 0, nb)
    loop(0, BEAM // (2 * nb), step)


def shards(queries, beam_ids, child_table, w_query, w_child, w_cross, bias, w_out):
    qd, width = beam_ids.shape
    embed = queries.shape[1]
    half = child_table.shape[0] // 2
    hid_dev = w_query.shape[1]
    share = 3 * qd * width // (2 * BEAM * HID)
    nb = 2
    ints = pltpu.VMEM((qd, width), I32)
    floats = pltpu.VMEM((qd, width), F32)

    rank, req_all, q_all, w_all, vec_all, buf = pl.pallas_call(
        functools.partial(front_kernel, share),
        out_shape=(
            shape((qd, width), I32),
            pltpu.VMEM((BEAM, 4, 128), I32),
            pltpu.VMEM((BEAM * qd, embed), BF16),
            pltpu.VMEM((HID, 3, embed, hid_dev), BF16),
            pltpu.VMEM((HID, 2, hid_dev), F32),
            pltpu.VMEM((half, 2, embed), BF16),
        ),
        in_specs=[VM] + [ANY] * 7,
        out_specs=(VM,) * 6,
        scratch_shapes=[
            pltpu.VMEM((BEAM, 4, 128), I32),
            ints,
            ints,
            floats,
            floats,
            floats,
            dma(4),
            dma(6),
            *[dma(BEAM)] * 4,
            *[dma(HID)] * 2,
            dma(7),
            dma(HID),
            *[dma(HID)] * 2,
            *[dma(4)] * 2,
        ],
        compiler_params=pltpu.CompilerParams(collective_id=0, has_side_effects=True, vmem_limit_bytes=45 * 2**20),
        name="front",
    )(beam_ids, queries, w_query, w_child, w_cross, bias.reshape(1, -1), w_out.reshape(1, -1), child_table)

    scores = pl.pallas_call(
        functools.partial(score_kernel, share, nb, qd),
        out_shape=pltpu.VMEM((BEAM, 3, 128), F32),
        in_specs=[VM, pl.BlockSpec(memory_space=pltpu.SMEM)] + [VM] * 4,
        out_specs=VM,
        scratch_shapes=[*[pltpu.VMEM((nb * share, 2, embed), BF16)] * 2, pltpu.VMEM((BEAM, 2 * share), I32)],
        compiler_params=pltpu.CompilerParams(vmem_limit_bytes=20 * 2**20),
        name="score",
    )(req_all, req_all, q_all, w_all, vec_all, buf)

    sall = pl.pallas_call(
        back_kernel,
        out_shape=pltpu.VMEM((HID, BEAM, 3, 128), F32),
        in_specs=[VM],
        out_specs=VM,
        scratch_shapes=[dma(BEAM), dma(BEAM), dma(HID), dma(HID)],
        compiler_params=pltpu.CompilerParams(collective_id=1, has_side_effects=True, vmem_limit_bytes=8 * 2**20),
        name="give_back",
    )(scores)

    def place_kernel(ids, rank, sall, out):
        unpermute(lax.axis_index("hid"), HID, BEAM, share, half, ids, rank, sall, out)

    return pl.pallas_call(
        place_kernel,
        out_shape=shape((qd, 2 * width // HID), F32),
        in_specs=[VM] * 3,
        out_specs=VM,
        compiler_params=pltpu.CompilerParams(vmem_limit_bytes=24 * 2**20),
        name="place",
    )(beam_ids, rank, sall)


def solution(mesh):
    return jax.shard_map(
        shards,
        mesh=mesh,
        in_specs=(
            P("beam", None),
            P("beam", None),
            P("beam", None),
            P(None, "hid"),
            P(None, "hid"),
            P(None, "hid"),
            P("hid"),
            P("hid"),
        ),
        out_specs=P("beam", "hid"),
        check_vma=False,
    )
```

```python
import functools
import math

import jax
import jax.numpy as jnp
from jax import lax
from jax.experimental import pallas as pl
from jax.experimental.pallas import tpu as pltpu
from jax.sharding import PartitionSpec as P

F32, BF16, I32 = jnp.float32, jnp.bfloat16, jnp.int32
NT = (((1,), (1,)), ((), ()))
TN = (((0,), (0,)), ((), ()))


def iota(shape, dim):
    return lax.broadcasted_iota(I32, shape, dim)


def route(h, nbeam, share, half, midway, ids_ref, req_ref, rank_ref, a_ref, c_ref, v0_ref, v1_ref, q_ref):
    qd, width = ids_ref.shape
    lo = ids_ref[:, :128]
    hi = ids_ref[:, 128:]
    ids = jnp.concatenate([lo, hi], axis=0)
    rows = ids.shape[0]
    owner = ids // half
    before_lane = (iota((128, 128), 0) < iota((128, 128), 1)).astype(BF16)
    ones = jnp.ones((128, 128), BF16)
    both = jnp.concatenate([before_lane, ones], axis=1)
    before_row = (iota((rows, rows), 1) < iota((rows, rows), 0)).astype(BF16)
    rank = jnp.zeros((rows, 128), F32)
    for o in range(nbeam):
        hit = owner == o
        counts = jnp.dot(hit.astype(BF16), both, preferred_element_type=F32)
        above = jnp.dot(before_row, counts[:, 128:].astype(BF16), preferred_element_type=F32)
        rank = rank + jnp.where(hit, counts[:, :128] + above, 0.0)
    rank = rank.astype(I32)
    rank = jnp.concatenate([rank[:qd], rank[qd:]], axis=1)
    rank_ref[...] = rank
    ids = ids_ref[...]
    owner = ids // half
    offset = ids - owner * half
    local = rank - h * share
    place = owner * 256 + local
    inside = (local >= 0) & (local < share)
    a_ref[...] = jnp.where(inside, place // 128, -1)
    c_ref[...] = place % 128
    v0_ref[...] = (offset % 128).astype(F32)
    v1_ref[...] = (offset // 128).astype(F32)
    q_ref[...] = iota((qd, width), 0).astype(F32)
    na = 2 * nbeam
    arow = iota((na, width), 0)
    crow = iota((128, width), 0)

    def step(r, total):
        one = pl.ds(r, 1)
        hit = arow == a_ref[one, :]
        left = jnp.concatenate([jnp.where(hit, ref[one, :], 0.0) for ref in (v0_ref, v1_ref, q_ref)], axis=0)
        right = (crow == c_ref[one, :]).astype(F32)
        return total + lax.dot_general(left.astype(BF16), right.astype(BF16), NT, preferred_element_type=F32)

    table = lax.fori_loop(0, qd // 2, step, jnp.zeros((3 * na, 128), F32), unroll=8)
    midway()
    table = lax.fori_loop(qd // 2, qd, step, table, unroll=8).astype(I32)
    offs = table[:na] + 128 * table[na : 2 * na]
    qs = table[2 * na :]
    for o in range(nbeam):
        req_ref[o, 0:2, :] = offs[2 * o : 2 * o + 2]
        req_ref[o, 2:4, :] = qs[2 * o : 2 * o + 2]


def table_copies(table_ref, buf_ref, sems):
    groups = table_ref.shape[0] // 8
    width = table_ref.shape[1]
    src = table_ref.reshape(groups, 8, width)
    dst = buf_ref.reshape(groups, 4, 2, width)
    return [pltpu.make_async_copy(src.at[:, 2 * p : 2 * p + 2, :], dst.at[:, p], sems.at[p]) for p in range(4)]


def gather(share, off_ref, buf_ref, rows_ref, first, count):
    for i in range(count):
        for k in range(share):
            rows_ref[i * share + k] = buf_ref[off_ref[first + i, k // 128, k % 128]]


def split2(x):
    hi = x.astype(BF16)
    return hi, (x - hi.astype(F32)).astype(BF16)


def score(share, b0, nb, qd, twice_ref, rows_ref, queries_ref, wq_ref, wc_ref, wx_ref, vec_ref, out_ref):
    shards = wq_ref.shape[0]
    width = queries_ref.shape[1]
    m = nb * 2 * share
    qrows = []
    for i in range(nb):
        b = b0 + i
        oht = (iota((qd, 2 * share), 0) == twice_ref[pl.ds(b, 1), :]).astype(F32).astype(BF16)
        qb = queries_ref[pl.ds(pl.multiple_of(b * qd, qd), qd), :]
        qrows.append(lax.dot_general(oht, qb, TN, preferred_element_type=F32).astype(BF16))
    qrow = jnp.concatenate(qrows, axis=0) if nb > 1 else qrows[0]
    child = rows_ref[...].reshape(m, width)
    cross = child * qrow
    acc = jnp.zeros((m, 128), F32)
    for n in range(0, shards, 2):
        pair = lambda ref: jnp.concatenate([ref[n], ref[n + 1]], axis=1)
        pre = jnp.dot(child, pair(wc_ref), preferred_element_type=F32)
        pre += jnp.dot(cross, pair(wx_ref), preferred_element_type=F32)
        pre += jnp.dot(qrow, pair(wq_ref), preferred_element_type=F32)
        for j in range(2):
            part = pre[:, 128 * j : 128 * j + 128]
            acc += jnp.maximum(part + vec_ref[n + j, 0:1, :], 0.0) * vec_ref[n + j, 1:2, :]
    total = acc.T
    total = jnp.sum(total, axis=0, keepdims=True)
    for i in range(nb):
        for t in range(2 * share // 128):
            lo = i * 2 * share + t * 128
            out_ref[b0 + i, t : t + 1, :] = total[:, lo : lo + 128]


def unpermute(h, nhid, nbeam, share, half, ids_ref, rank_ref, sall_ref, out_ref):
    qd, width = ids_ref.shape
    per = width // nhid

    def own(x):
        mine = jnp.zeros((qd, per), I32)
        for k in range(nhid):
            mine = jnp.where(h == k, x[:, k * per : (k + 1) * per], mine)
        return jnp.concatenate([mine[8 * g : 8 * g + 8] for g in range(qd // 8)], axis=1)

    owner = own(ids_ref[...]) // half
    rank = own(rank_ref[...])
    chunk = rank // share
    local = rank - chunk * share
    tiles = 2 * share // 128
    row = (chunk * nbeam + owner) * tiles + local // 64
    lane = (local % 64) * 2
    nrows = nhid * nbeam * tiles
    scores = sall_ref[...].reshape(nrows, 128).T
    hi, lo = split2(scores)
    parts = jnp.concatenate([hi, lo], axis=0)
    lanes = lane.shape[1]
    rio = iota((nrows, lanes), 0)
    cio = iota((128, lanes), 0)
    evens, odds = [], []
    for i in range(8):
        onehot = (rio == row[i : i + 1]).astype(F32).astype(BF16)
        got = jnp.dot(parts, onehot, preferred_element_type=F32)
        got = got[:128] + got[128:]
        evens.append(jnp.sum(jnp.where(cio == lane[i : i + 1], got, 0.0), axis=0, keepdims=True))
        odds.append(jnp.sum(jnp.where(cio == lane[i : i + 1] + 1, got, 0.0), axis=0, keepdims=True))
    even = jnp.concatenate(split2(jnp.concatenate(evens, axis=0)), axis=0)
    odd = jnp.concatenate(split2(jnp.concatenate(odds, axis=0)), axis=0)
    n = iota((lanes, 2 * lanes), 1)
    k = iota((lanes, 2 * lanes), 0)
    mixed = jnp.dot(even, (n == 2 * k).astype(BF16), preferred_element_type=F32)
    mixed += jnp.dot(odd, (n == 2 * k + 1).astype(BF16), preferred_element_type=F32)
    mixed = mixed[:8] + mixed[8:]
    for g in range(qd // 8):
        out_ref[8 * g : 8 * g + 8, :] = mixed[:, 2 * per * g : 2 * per * (g + 1)]


BEAM, HID = 16, 8
MESH = pl.DeviceIdType.MESH
VM = pl.BlockSpec(memory_space=pltpu.VMEM)
ANY = pl.BlockSpec(memory_space=pltpu.HBM)


def shape(dims, dtype):
    return jax.ShapeDtypeStruct(dims, dtype)


def dma(*dims):
    return pltpu.SemaphoreType.DMA(dims)


def remote(src, dst, send, recv, device):
    return pltpu.make_async_remote_copy(
        src_ref=src, dst_ref=dst, send_sem=send, recv_sem=recv, device_id=device, device_id_type=MESH
    )


def loop(lo, hi, body):
    def step(i, _):
        body(i)
        return 0

    lax.fori_loop(lo, hi, step, 0)


def front_kernel(
    share,
    ids,
    queries,
    wq,
    wc,
    wx,
    bias,
    w_out,
    table,
    rank,
    req_all,
    q_all,
    w_all,
    vec_all,
    buf,
    req,
    a_ref,
    c_ref,
    v0_ref,
    v1_ref,
    qi_ref,
    table_sem,
    own_sem,
    rsend,
    rrecv,
    qsend,
    qrecv,
    msend,
    vsend,
    vrecv,
    wsend,
    wrecv,
    psend,
    precv,
    fsend,
    frecv,
):
    b, h = lax.axis_index("beam"), lax.axis_index("hid")
    core = lax.rem(b, 2)
    mate = b + 1 - 2 * core
    z = lax.rem(h, 2)
    across = h + 1 - 2 * z
    beyond = lax.rem(b + BEAM // 2, BEAM)
    qd = ids.shape[0]
    half = table.shape[0] // 2
    depth = w_all.shape[2] // 2

    def beam_peer(j):
        return lax.rem(b + j, BEAM)

    def hid_peer(j):
        return lax.rem(h + j, HID)

    def x_peer(j):
        return lax.rem(h + 2 * j, HID)

    barrier = pltpu.get_barrier_semaphore()
    loop(1, BEAM, lambda j: pl.semaphore_signal(barrier, inc=1, device_id=(beam_peer(j), h), device_id_type=MESH))
    loop(1, HID, lambda j: pl.semaphore_signal(barrier, inc=1, device_id=(b, hid_peer(j)), device_id_type=MESH))
    pl.semaphore_signal(barrier, inc=1, device_id=(beyond, across), device_id_type=MESH)

    def q_rows(i):
        return pl.ds(pl.multiple_of(i * qd, qd), qd)

    own = [
        pltpu.make_async_copy(src, w_all.at[h, i], own_sem.at[i]) for i, src in enumerate((wq, wc, wx))
    ]
    own.append(pltpu.make_async_copy(queries, q_all.at[q_rows(b), :], own_sem.at[3]))
    own.append(pltpu.make_async_copy(bias, vec_all.at[h, 0:1, :], own_sem.at[4]))
    own.append(pltpu.make_async_copy(w_out, vec_all.at[h, 1:2, :], own_sem.at[5]))
    for copy in own:
        copy.start()
    pulls = table_copies(table, buf, table_sem)
    for copy in pulls:
        copy.start()
    for copy in own:
        copy.wait()
    pl.semaphore_wait(barrier, BEAM + HID - 1)

    def piece(shard, part):
        return w_all.at[shard, :, pl.ds(pl.multiple_of(part * depth, depth), depth), :]

    def w_copy(shard, to, slot):
        return remote(piece(shard, core), piece(shard, core), wsend.at[slot], wrecv.at[shard], (b, to))

    def z_copy(shard):
        return remote(piece(shard, core), piece(shard, core), wsend.at[0], wrecv.at[shard], (beyond, across))

    def quarter(shard, side):
        start = pl.multiple_of(core * depth + side * (depth // 2), depth // 2)
        return w_all.at[shard, :, pl.ds(start, depth // 2), :]

    def pass_on(shard, side, lane):
        part = quarter(shard, side)
        return remote(part, part, fsend.at[lane + side], frecv.at[lane + side], (b, x_peer(3 - 2 * side)))

    beside = [x_peer(j) for j in (1, 3)]
    near = [lax.rem(across + 2 * j, HID) for j in (1, 3)]
    ends = (x_peer(2), lax.rem(across + 4, HID))

    def mate_copy(shard):
        return remote(piece(shard, core), piece(shard, core), psend.at[shard], precv.at[shard], (mate, h))

    def mate_arrival(shard):
        other = piece(shard, 1 - core)
        return remote(other, other, psend.at[shard], precv.at[shard], (mate, h))

    def q_copy(to, slot):
        return remote(q_all.at[q_rows(slot), :], q_all.at[q_rows(slot), :], qsend.at[to], qrecv.at[slot], (to, h))

    def q_mate(slot):
        return remote(q_all.at[q_rows(slot), :], q_all.at[q_rows(slot), :], msend.at[slot], qrecv.at[slot], (mate, h))

    def twin(j):
        return lax.rem(b + 2 * j, BEAM)

    def mates_twin(j):
        return lax.rem(mate + 2 * j, BEAM)

    def v_copy(to, slot):
        return remote(vec_all.at[slot], vec_all.at[slot], vsend.at[to], vrecv.at[slot], (b, to))

    def r_copy(to, slot):
        return remote(req.at[to], req_all.at[slot], rsend.at[to], rrecv.at[slot], (to, h))

    z_copy(h).start()
    for j in (1, 3):
        w_copy(h, x_peer(j), j).start()
    loop(1, HID, lambda j: v_copy(hid_peer(j), h).start())
    loop(1, BEAM // 2, lambda j: q_copy(twin(j), b).start())
    q_mate(b).start()

    def midway():
        z_copy(across).wait_recv()
        for j in (1, 3):
            w_copy(across, x_peer(j), 3 + j).start()
        for side, shard in enumerate(beside):
            w_copy(shard, shard, 0).wait_recv()
            pass_on(shard, side, 0).start()
        mate_copy(across).start()
        for shard in beside:
            mate_copy(shard).start()

    route(h, BEAM, share, half, midway, ids, req, rank, a_ref, c_ref, v0_ref, v1_ref, qi_ref)
    loop(1, BEAM, lambda j: r_copy(beam_peer(j), b).start())
    req_all[pl.ds(b, 1)] = req[pl.ds(b, 1)]

    def hand_over(j):
        q_copy(twin(j), twin(j)).wait_recv()
        q_mate(twin(j)).start()

    loop(1, BEAM // 2, hand_over)


    for side, shard in enumerate(near):
        w_copy(shard, shard, 0).wait_recv()
        pass_on(shard, side, 2).start()
        mate_copy(shard).start()
    for i, shard in enumerate(ends):
        for side in range(2):
            pass_on(shard, side, 2 * i).wait_recv()
        mate_copy(shard).start()
    loop(1, BEAM, lambda j: r_copy(beam_peer(j), beam_peer(j)).wait_recv())
    for copy in pulls:
        copy.wait()
    loop(0, BEAM // 2, lambda j: q_mate(mates_twin(j)).wait_recv())
    loop(1, HID, lambda j: v_copy(hid_peer(j), hid_peer(j)).wait_recv())
    loop(1, HID, lambda j: mate_arrival(hid_peer(j)).wait_recv())

    z_copy(h).wait_send()
    for j in (1, 3):
        w_copy(h, x_peer(j), j).wait_send()
        w_copy(across, x_peer(j), 3 + j).wait_send()
    for i, pair in enumerate((beside, near)):
        for side, shard in enumerate(pair):
            pass_on(shard, side, 2 * i).wait_send()
    loop(1, BEAM // 2, lambda j: q_copy(twin(j), b).wait_send())
    loop(0, BEAM // 2, lambda j: q_mate(twin(j)).wait_send())
    loop(1, BEAM, lambda j: r_copy(beam_peer(j), b).wait_send())
    loop(1, HID, lambda j: v_copy(hid_peer(j), h).wait_send())
    loop(1, HID, lambda j: mate_copy(hid_peer(j)).wait_send())


def back_kernel(scores, sall, bsend, brecv, hsend, hrecv):
    b, h = lax.axis_index("beam"), lax.axis_index("hid")

    def beam_peer(j):
        return lax.rem(b + j, BEAM)

    def hid_peer(j):
        return lax.rem(h + j, HID)

    barrier = pltpu.get_barrier_semaphore()
    loop(1, BEAM, lambda j: pl.semaphore_signal(barrier, inc=1, device_id=(beam_peer(j), h), device_id_type=MESH))
    loop(1, HID, lambda j: pl.semaphore_signal(barrier, inc=1, device_id=(b, hid_peer(j)), device_id_type=MESH))
    pl.semaphore_wait(barrier, BEAM + HID - 2)

    def back(to, slot):
        return remote(scores.at[to], sall.at[h, slot], bsend.at[to], brecv.at[slot], (to, h))

    def spread(to, slot):
        return remote(sall.at[slot], sall.at[slot], hsend.at[to], hrecv.at[slot], (b, to))

    loop(1, BEAM, lambda j: back(beam_peer(j), b).start())
    sall[h, pl.ds(b, 1)] = scores[pl.ds(b, 1)]
    loop(1, BEAM, lambda j: back(beam_peer(j), beam_peer(j)).wait_recv())
    loop(1, HID, lambda j: spread(hid_peer(j), h).start())
    loop(1, BEAM, lambda j: back(beam_peer(j), b).wait_send())
    loop(1, HID, lambda j: spread(hid_peer(j), h).wait_send())
    loop(1, HID, lambda j: spread(hid_peer(j), hid_peer(j)).wait_recv())


def score_kernel(share, nb, qd, req, off, queries, w_all, vec, buf, scores, rows, rows2, twice):
    lists = req[...]
    qs = jnp.concatenate([lists[:, 2, :], lists[:, 3, : share - 128]], axis=1).astype(F32).astype(BF16)
    dup = (iota((share, 2 * share), 1) // 2 == iota((share, 2 * share), 0)).astype(F32).astype(BF16)
    twice[...] = jnp.dot(qs, dup, preferred_element_type=F32).astype(I32)

    def run(first, now, then):
        gather(share, off, buf, then, jnp.minimum(first + nb, BEAM - nb), nb)
        score(share, first, nb, qd, twice, now, queries, w_all.at[:, 0], w_all.at[:, 1], w_all.at[:, 2], vec, scores)

    def step(i):
        run(2 * i * nb, rows, rows2)
        run((2 * i + 1) * nb, rows2, rows)

    gather(share, off, buf, rows, 0, nb)
    loop(0, BEAM // (2 * nb), step)


def shards(queries, beam_ids, child_table, w_query, w_child, w_cross, bias, w_out):
    qd, width = beam_ids.shape
    embed = queries.shape[1]
    half = child_table.shape[0] // 2
    hid_dev = w_query.shape[1]
    share = 3 * qd * width // (2 * BEAM * HID)
    nb = 2
    ints = pltpu.VMEM((qd, width), I32)
    floats = pltpu.VMEM((qd, width), F32)

    rank, req_all, q_all, w_all, vec_all, buf = pl.pallas_call(
        functools.partial(front_kernel, share),
        out_shape=(
            shape((qd, width), I32),
            pltpu.VMEM((BEAM, 4, 128), I32),
            pltpu.VMEM((BEAM * qd, embed), BF16),
            pltpu.VMEM((HID, 3, embed, hid_dev), BF16),
            pltpu.VMEM((HID, 2, hid_dev), F32),
            pltpu.VMEM((half, 2, embed), BF16),
        ),
        in_specs=[VM] + [ANY] * 7,
        out_specs=(VM,) * 6,
        scratch_shapes=[
            pltpu.VMEM((BEAM, 4, 128), I32),
            ints,
            ints,
            floats,
            floats,
            floats,
            dma(4),
            dma(6),
            *[dma(BEAM)] * 5,
            *[dma(HID)] * 2,
            dma(7),
            dma(HID),
            *[dma(HID)] * 2,
            *[dma(4)] * 2,
        ],
        compiler_params=pltpu.CompilerParams(collective_id=0, has_side_effects=True, vmem_limit_bytes=45 * 2**20),
        name="front",
    )(beam_ids, queries, w_query, w_child, w_cross, bias.reshape(1, -1), w_out.reshape(1, -1), child_table)

    scores = pl.pallas_call(
        functools.partial(score_kernel, share, nb, qd),
        out_shape=pltpu.VMEM((BEAM, 3, 128), F32),
        in_specs=[VM, pl.BlockSpec(memory_space=pltpu.SMEM)] + [VM] * 4,
        out_specs=VM,
        scratch_shapes=[*[pltpu.VMEM((nb * share, 2, embed), BF16)] * 2, pltpu.VMEM((BEAM, 2 * share), I32)],
        compiler_params=pltpu.CompilerParams(vmem_limit_bytes=20 * 2**20),
        name="score",
    )(req_all, req_all, q_all, w_all, vec_all, buf)

    sall = pl.pallas_call(
        back_kernel,
        out_shape=pltpu.VMEM((HID, BEAM, 3, 128), F32),
        in_specs=[VM],
        out_specs=VM,
        scratch_shapes=[dma(BEAM), dma(BEAM), dma(HID), dma(HID)],
        compiler_params=pltpu.CompilerParams(collective_id=1, has_side_effects=True, vmem_limit_bytes=8 * 2**20),
        name="give_back",
    )(scores)

    def place_kernel(ids, rank, sall, out):
        unpermute(lax.axis_index("hid"), HID, BEAM, share, half, ids, rank, sall, out)

    return pl.pallas_call(
        place_kernel,
        out_shape=shape((qd, 2 * width // HID), F32),
        in_specs=[VM] * 3,
        out_specs=VM,
        compiler_params=pltpu.CompilerParams(vmem_limit_bytes=24 * 2**20),
        name="place",
    )(beam_ids, rank, sall)


def solution(mesh):
    return jax.shard_map(
        shards,
        mesh=mesh,
        in_specs=(
            P("beam", None),
            P("beam", None),
            P("beam", None),
            P(None, "hid"),
            P(None, "hid"),
            P(None, "hid"),
            P("hid"),
            P("hid"),
        ),
        out_specs=P("beam", "hid"),
        check_vma=False,
    )
```

```python
import functools
import math

import jax
import jax.numpy as jnp
from jax import lax
from jax.experimental import pallas as pl
from jax.experimental.pallas import tpu as pltpu
from jax.sharding import PartitionSpec as P

F32, BF16, I32 = jnp.float32, jnp.bfloat16, jnp.int32
NT = (((1,), (1,)), ((), ()))
TN = (((0,), (0,)), ((), ()))


def iota(shape, dim):
    return lax.broadcasted_iota(I32, shape, dim)


def route(h, nbeam, share, half, ranked, midway, ids_ref, req_ref, rank_ref, a_ref, c_ref, v0_ref, v1_ref, q_ref):
    qd, width = ids_ref.shape
    lo = ids_ref[:, :128]
    hi = ids_ref[:, 128:]
    ids = jnp.concatenate([lo, hi], axis=0)
    rows = ids.shape[0]
    owner = ids // half
    before_lane = (iota((128, 128), 0) < iota((128, 128), 1)).astype(BF16)
    ones = jnp.ones((128, 128), BF16)
    both = jnp.concatenate([before_lane, ones], axis=1)
    before_row = (iota((rows, rows), 1) < iota((rows, rows), 0)).astype(BF16)
    rank = jnp.zeros((rows, 128), F32)
    for o in range(nbeam):
        hit = owner == o
        counts = jnp.dot(hit.astype(BF16), both, preferred_element_type=F32)
        above = jnp.dot(before_row, counts[:, 128:].astype(BF16), preferred_element_type=F32)
        rank = rank + jnp.where(hit, counts[:, :128] + above, 0.0)
    rank = rank.astype(I32)
    rank = jnp.concatenate([rank[:qd], rank[qd:]], axis=1)
    rank_ref[...] = rank
    ranked()
    ids = ids_ref[...]
    owner = ids // half
    offset = ids - owner * half
    local = rank - h * share
    place = owner * 256 + local
    inside = (local >= 0) & (local < share)
    a_ref[...] = jnp.where(inside, place // 128, -1)
    c_ref[...] = place % 128
    v0_ref[...] = (offset % 128).astype(F32)
    v1_ref[...] = (offset // 128).astype(F32)
    q_ref[...] = iota((qd, width), 0).astype(F32)
    na = 2 * nbeam
    arow = iota((na, width), 0)
    crow = iota((128, width), 0)

    def step(r, total):
        one = pl.ds(r, 1)
        hit = arow == a_ref[one, :]
        left = jnp.concatenate([jnp.where(hit, ref[one, :], 0.0) for ref in (v0_ref, v1_ref, q_ref)], axis=0)
        right = (crow == c_ref[one, :]).astype(F32)
        return total + lax.dot_general(left.astype(BF16), right.astype(BF16), NT, preferred_element_type=F32)

    table = lax.fori_loop(0, qd // 2, step, jnp.zeros((3 * na, 128), F32), unroll=8)
    midway()
    table = lax.fori_loop(qd // 2, qd, step, table, unroll=8).astype(I32)
    offs = table[:na] + 128 * table[na : 2 * na]
    qs = table[2 * na :]
    for o in range(nbeam):
        req_ref[o, 0:2, :] = offs[2 * o : 2 * o + 2]
        req_ref[o, 2:4, :] = qs[2 * o : 2 * o + 2]


def table_copies(table_ref, buf_ref, sems):
    groups = table_ref.shape[0] // 8
    width = table_ref.shape[1]
    src = table_ref.reshape(groups, 8, width)
    dst = buf_ref.reshape(groups, 4, 2, width)
    return [pltpu.make_async_copy(src.at[:, 2 * p : 2 * p + 2, :], dst.at[:, p], sems.at[p]) for p in range(4)]


def gather(share, off_ref, buf_ref, rows_ref, first, count):
    for i in range(count):
        for k in range(share):
            rows_ref[i * share + k] = buf_ref[off_ref[first + i, k // 128, k % 128]]


def split2(x):
    hi = x.astype(BF16)
    return hi, (x - hi.astype(F32)).astype(BF16)


def score(share, b0, nb, qd, twice_ref, rows_ref, queries_ref, wq_ref, wc_ref, wx_ref, vec_ref, out_ref):
    shards = wq_ref.shape[0]
    width = queries_ref.shape[1]
    m = nb * 2 * share
    qrows = []
    for i in range(nb):
        b = b0 + i
        oht = (iota((qd, 2 * share), 0) == twice_ref[pl.ds(b, 1), :]).astype(F32).astype(BF16)
        qb = queries_ref[pl.ds(pl.multiple_of(b * qd, qd), qd), :]
        qrows.append(lax.dot_general(oht, qb, TN, preferred_element_type=F32).astype(BF16))
    qrow = jnp.concatenate(qrows, axis=0) if nb > 1 else qrows[0]
    child = rows_ref[...].reshape(m, width)
    cross = child * qrow
    acc = jnp.zeros((m, 128), F32)
    for n in range(0, shards, 2):
        pair = lambda ref: jnp.concatenate([ref[n], ref[n + 1]], axis=1)
        pre = jnp.dot(child, pair(wc_ref), preferred_element_type=F32)
        pre += jnp.dot(cross, pair(wx_ref), preferred_element_type=F32)
        pre += jnp.dot(qrow, pair(wq_ref), preferred_element_type=F32)
        for j in range(2):
            part = pre[:, 128 * j : 128 * j + 128]
            acc += jnp.maximum(part + vec_ref[n + j, 0:1, :], 0.0) * vec_ref[n + j, 1:2, :]
    total = acc.T
    total = jnp.sum(total, axis=0, keepdims=True)
    for i in range(nb):
        for t in range(2 * share // 128):
            lo = i * 2 * share + t * 128
            out_ref[b0 + i, t : t + 1, :] = total[:, lo : lo + 128]


def unpermute(h, nhid, nbeam, share, half, ids_ref, rank_ref, sall_ref, out_ref):
    qd, width = ids_ref.shape
    per = width // nhid

    def own(x):
        mine = jnp.zeros((qd, per), I32)
        for k in range(nhid):
            mine = jnp.where(h == k, x[:, k * per : (k + 1) * per], mine)
        return jnp.concatenate([mine[8 * g : 8 * g + 8] for g in range(qd // 8)], axis=1)

    owner = own(ids_ref[...]) // half
    rank = own(rank_ref[...])
    chunk = rank // share
    local = rank - chunk * share
    tiles = 2 * share // 128
    row = (chunk * nbeam + owner) * tiles + local // 64
    lane = (local % 64) * 2
    nrows = nhid * nbeam * tiles
    scores = sall_ref[...].reshape(nrows, 128).T
    hi, lo = split2(scores)
    parts = jnp.concatenate([hi, lo], axis=0)
    lanes = lane.shape[1]
    rio = iota((nrows, lanes), 0)
    cio = iota((128, lanes), 0)
    evens, odds = [], []
    for i in range(8):
        onehot = (rio == row[i : i + 1]).astype(F32).astype(BF16)
        got = jnp.dot(parts, onehot, preferred_element_type=F32)
        got = got[:128] + got[128:]
        evens.append(jnp.sum(jnp.where(cio == lane[i : i + 1], got, 0.0), axis=0, keepdims=True))
        odds.append(jnp.sum(jnp.where(cio == lane[i : i + 1] + 1, got, 0.0), axis=0, keepdims=True))
    even = jnp.concatenate(split2(jnp.concatenate(evens, axis=0)), axis=0)
    odd = jnp.concatenate(split2(jnp.concatenate(odds, axis=0)), axis=0)
    n = iota((lanes, 2 * lanes), 1)
    k = iota((lanes, 2 * lanes), 0)
    mixed = jnp.dot(even, (n == 2 * k).astype(BF16), preferred_element_type=F32)
    mixed += jnp.dot(odd, (n == 2 * k + 1).astype(BF16), preferred_element_type=F32)
    mixed = mixed[:8] + mixed[8:]
    for g in range(qd // 8):
        out_ref[8 * g : 8 * g + 8, :] = mixed[:, 2 * per * g : 2 * per * (g + 1)]


BEAM, HID = 16, 8
MESH = pl.DeviceIdType.MESH
VM = pl.BlockSpec(memory_space=pltpu.VMEM)
ANY = pl.BlockSpec(memory_space=pltpu.HBM)


def shape(dims, dtype):
    return jax.ShapeDtypeStruct(dims, dtype)


def dma(*dims):
    return pltpu.SemaphoreType.DMA(dims)


def remote(src, dst, send, recv, device):
    return pltpu.make_async_remote_copy(
        src_ref=src, dst_ref=dst, send_sem=send, recv_sem=recv, device_id=device, device_id_type=MESH
    )


def loop(lo, hi, body):
    def step(i, _):
        body(i)
        return 0

    lax.fori_loop(lo, hi, step, 0)


def front_kernel(
    share,
    ids,
    queries,
    wq,
    wc,
    wx,
    bias,
    w_out,
    table,
    rank,
    req_all,
    q_all,
    w_all,
    vec_all,
    buf,
    req,
    a_ref,
    c_ref,
    v0_ref,
    v1_ref,
    qi_ref,
    table_sem,
    own_sem,
    rsend,
    rrecv,
    qsend,
    qrecv,
    msend,
    vsend,
    vrecv,
    wsend,
    wrecv,
    psend,
    precv,
    fsend,
    frecv,
):
    b, h = lax.axis_index("beam"), lax.axis_index("hid")
    core = lax.rem(b, 2)
    mate = b + 1 - 2 * core
    z = lax.rem(h, 2)
    across = h + 1 - 2 * z
    beyond = lax.rem(b + BEAM // 2, BEAM)
    qd = ids.shape[0]
    half = table.shape[0] // 2
    depth = w_all.shape[2] // 2

    def beam_peer(j):
        return lax.rem(b + j, BEAM)

    def hid_peer(j):
        return lax.rem(h + j, HID)

    def x_peer(j):
        return lax.rem(h + 2 * j, HID)

    barrier = pltpu.get_barrier_semaphore()
    loop(1, BEAM, lambda j: pl.semaphore_signal(barrier, inc=1, device_id=(beam_peer(j), h), device_id_type=MESH))
    loop(1, HID, lambda j: pl.semaphore_signal(barrier, inc=1, device_id=(b, hid_peer(j)), device_id_type=MESH))
    pl.semaphore_signal(barrier, inc=1, device_id=(beyond, across), device_id_type=MESH)

    def q_rows(i):
        return pl.ds(pl.multiple_of(i * qd, qd), qd)

    own = [
        pltpu.make_async_copy(src, w_all.at[h, i], own_sem.at[i]) for i, src in enumerate((wq, wc, wx))
    ]
    own.append(pltpu.make_async_copy(queries, q_all.at[q_rows(b), :], own_sem.at[3]))
    own.append(pltpu.make_async_copy(bias, vec_all.at[h, 0:1, :], own_sem.at[4]))
    own.append(pltpu.make_async_copy(w_out, vec_all.at[h, 1:2, :], own_sem.at[5]))
    for copy in own:
        copy.start()
    pulls = table_copies(table, buf, table_sem)
    for copy in pulls:
        copy.start()
    def piece(shard, part):
        return w_all.at[shard, :, pl.ds(pl.multiple_of(part * depth, depth), depth), :]

    def w_copy(shard, to, slot):
        return remote(piece(shard, core), piece(shard, core), wsend.at[slot], wrecv.at[shard], (b, to))

    def z_copy(shard):
        return remote(piece(shard, core), piece(shard, core), wsend.at[0], wrecv.at[shard], (beyond, across))

    def quarter(shard, side):
        start = pl.multiple_of(core * depth + side * (depth // 2), depth // 2)
        return w_all.at[shard, :, pl.ds(start, depth // 2), :]

    def pass_on(shard, side, lane):
        part = quarter(shard, side)
        return remote(part, part, fsend.at[lane + side], frecv.at[lane + side], (b, x_peer(3 - 2 * side)))

    beside = [x_peer(j) for j in (1, 3)]
    near = [lax.rem(across + 2 * j, HID) for j in (1, 3)]
    ends = (x_peer(2), lax.rem(across + 4, HID))

    def mate_copy(shard):
        return remote(piece(shard, core), piece(shard, core), psend.at[shard], precv.at[shard], (mate, h))

    def mate_arrival(shard):
        other = piece(shard, 1 - core)
        return remote(other, other, psend.at[shard], precv.at[shard], (mate, h))

    def q_copy(to, slot):
        return remote(q_all.at[q_rows(slot), :], q_all.at[q_rows(slot), :], qsend.at[to], qrecv.at[slot], (to, h))

    def q_mate(slot):
        return remote(q_all.at[q_rows(slot), :], q_all.at[q_rows(slot), :], msend.at[slot], qrecv.at[slot], (mate, h))

    def twin(j):
        return lax.rem(b + 2 * j, BEAM)

    def mates_twin(j):
        return lax.rem(mate + 2 * j, BEAM)

    def v_copy(to, slot):
        return remote(vec_all.at[slot], vec_all.at[slot], vsend.at[to], vrecv.at[slot], (b, to))

    def r_copy(to, slot):
        return remote(req.at[to], req_all.at[slot], rsend.at[to], rrecv.at[slot], (to, h))

    def ranked():
        for copy in own:
            copy.wait()
        pl.semaphore_wait(barrier, BEAM + HID - 1)
        z_copy(h).start()
        for j in (1, 3):
            w_copy(h, x_peer(j), j).start()
        loop(1, HID, lambda j: v_copy(hid_peer(j), h).start())
        loop(1, BEAM // 2, lambda j: q_copy(twin(j), b).start())
        q_mate(b).start()

    def midway():
        z_copy(across).wait_recv()
        for j in (1, 3):
            w_copy(across, x_peer(j), 3 + j).start()
        mate_copy(across).start()

    route(h, BEAM, share, half, ranked, midway, ids, req, rank, a_ref, c_ref, v0_ref, v1_ref, qi_ref)
    loop(1, BEAM, lambda j: r_copy(beam_peer(j), b).start())
    req_all[pl.ds(b, 1)] = req[pl.ds(b, 1)]

    for side, shard in enumerate(beside):
        w_copy(shard, shard, 0).wait_recv()
        pass_on(shard, side, 0).start()
        mate_copy(shard).start()

    def hand_over(j):
        q_copy(twin(j), twin(j)).wait_recv()
        q_mate(twin(j)).start()

    loop(1, BEAM // 2, hand_over)


    for side, shard in enumerate(near):
        w_copy(shard, shard, 0).wait_recv()
        pass_on(shard, side, 2).start()
        mate_copy(shard).start()
    for i, shard in enumerate(ends):
        for side in range(2):
            pass_on(shard, side, 2 * i).wait_recv()
        mate_copy(shard).start()
    loop(1, BEAM, lambda j: r_copy(beam_peer(j), beam_peer(j)).wait_recv())
    for copy in pulls:
        copy.wait()
    loop(0, BEAM // 2, lambda j: q_mate(mates_twin(j)).wait_recv())
    loop(1, HID, lambda j: v_copy(hid_peer(j), hid_peer(j)).wait_recv())
    loop(1, HID, lambda j: mate_arrival(hid_peer(j)).wait_recv())

    z_copy(h).wait_send()
    for j in (1, 3):
        w_copy(h, x_peer(j), j).wait_send()
        w_copy(across, x_peer(j), 3 + j).wait_send()
    for i, pair in enumerate((beside, near)):
        for side, shard in enumerate(pair):
            pass_on(shard, side, 2 * i).wait_send()
    loop(1, BEAM // 2, lambda j: q_copy(twin(j), b).wait_send())
    loop(0, BEAM // 2, lambda j: q_mate(twin(j)).wait_send())
    loop(1, BEAM, lambda j: r_copy(beam_peer(j), b).wait_send())
    loop(1, HID, lambda j: v_copy(hid_peer(j), h).wait_send())
    loop(1, HID, lambda j: mate_copy(hid_peer(j)).wait_send())


def back_kernel(scores, sall, bsend, brecv, hsend, hrecv):
    b, h = lax.axis_index("beam"), lax.axis_index("hid")

    def beam_peer(j):
        return lax.rem(b + j, BEAM)

    def hid_peer(j):
        return lax.rem(h + j, HID)

    barrier = pltpu.get_barrier_semaphore()
    loop(1, BEAM, lambda j: pl.semaphore_signal(barrier, inc=1, device_id=(beam_peer(j), h), device_id_type=MESH))
    loop(1, HID, lambda j: pl.semaphore_signal(barrier, inc=1, device_id=(b, hid_peer(j)), device_id_type=MESH))
    pl.semaphore_wait(barrier, BEAM + HID - 2)

    def back(to, slot):
        return remote(scores.at[to], sall.at[h, slot], bsend.at[to], brecv.at[slot], (to, h))

    def spread(to, slot):
        return remote(sall.at[slot], sall.at[slot], hsend.at[to], hrecv.at[slot], (b, to))

    loop(1, BEAM, lambda j: back(beam_peer(j), b).start())
    sall[h, pl.ds(b, 1)] = scores[pl.ds(b, 1)]
    loop(1, BEAM, lambda j: back(beam_peer(j), beam_peer(j)).wait_recv())
    loop(1, HID, lambda j: spread(hid_peer(j), h).start())
    loop(1, BEAM, lambda j: back(beam_peer(j), b).wait_send())
    loop(1, HID, lambda j: spread(hid_peer(j), h).wait_send())
    loop(1, HID, lambda j: spread(hid_peer(j), hid_peer(j)).wait_recv())


def score_kernel(share, nb, qd, req, off, queries, w_all, vec, buf, scores, rows, rows2, twice):
    lists = req[...]
    qs = jnp.concatenate([lists[:, 2, :], lists[:, 3, : share - 128]], axis=1).astype(F32).astype(BF16)
    dup = (iota((share, 2 * share), 1) // 2 == iota((share, 2 * share), 0)).astype(F32).astype(BF16)
    twice[...] = jnp.dot(qs, dup, preferred_element_type=F32).astype(I32)

    def run(first, now, then):
        gather(share, off, buf, then, jnp.minimum(first + nb, BEAM - nb), nb)
        score(share, first, nb, qd, twice, now, queries, w_all.at[:, 0], w_all.at[:, 1], w_all.at[:, 2], vec, scores)

    def step(i):
        run(2 * i * nb, rows, rows2)
        run((2 * i + 1) * nb, rows2, rows)

    gather(share, off, buf, rows, 0, nb)
    loop(0, BEAM // (2 * nb), step)


def shards(queries, beam_ids, child_table, w_query, w_child, w_cross, bias, w_out):
    qd, width = beam_ids.shape
    embed = queries.shape[1]
    half = child_table.shape[0] // 2
    hid_dev = w_query.shape[1]
    share = 3 * qd * width // (2 * BEAM * HID)
    nb = 2
    ints = pltpu.VMEM((qd, width), I32)
    floats = pltpu.VMEM((qd, width), F32)

    rank, req_all, q_all, w_all, vec_all, buf = pl.pallas_call(
        functools.partial(front_kernel, share),
        out_shape=(
            shape((qd, width), I32),
            pltpu.VMEM((BEAM, 4, 128), I32),
            pltpu.VMEM((BEAM * qd, embed), BF16),
            pltpu.VMEM((HID, 3, embed, hid_dev), BF16),
            pltpu.VMEM((HID, 2, hid_dev), F32),
            pltpu.VMEM((half, 2, embed), BF16),
        ),
        in_specs=[VM] + [ANY] * 7,
        out_specs=(VM,) * 6,
        scratch_shapes=[
            pltpu.VMEM((BEAM, 4, 128), I32),
            ints,
            ints,
            floats,
            floats,
            floats,
            dma(4),
            dma(6),
            *[dma(BEAM)] * 5,
            *[dma(HID)] * 2,
            dma(7),
            dma(HID),
            *[dma(HID)] * 2,
            *[dma(4)] * 2,
        ],
        compiler_params=pltpu.CompilerParams(collective_id=0, has_side_effects=True, vmem_limit_bytes=45 * 2**20),
        name="front",
    )(beam_ids, queries, w_query, w_child, w_cross, bias.reshape(1, -1), w_out.reshape(1, -1), child_table)

    scores = pl.pallas_call(
        functools.partial(score_kernel, share, nb, qd),
        out_shape=pltpu.VMEM((BEAM, 3, 128), F32),
        in_specs=[VM, pl.BlockSpec(memory_space=pltpu.SMEM)] + [VM] * 4,
        out_specs=VM,
        scratch_shapes=[*[pltpu.VMEM((nb * share, 2, embed), BF16)] * 2, pltpu.VMEM((BEAM, 2 * share), I32)],
        compiler_params=pltpu.CompilerParams(vmem_limit_bytes=20 * 2**20),
        name="score",
    )(req_all, req_all, q_all, w_all, vec_all, buf)

    sall = pl.pallas_call(
        back_kernel,
        out_shape=pltpu.VMEM((HID, BEAM, 3, 128), F32),
        in_specs=[VM],
        out_specs=VM,
        scratch_shapes=[dma(BEAM), dma(BEAM), dma(HID), dma(HID)],
        compiler_params=pltpu.CompilerParams(collective_id=1, has_side_effects=True, vmem_limit_bytes=8 * 2**20),
        name="give_back",
    )(scores)

    def place_kernel(ids, rank, sall, out):
        unpermute(lax.axis_index("hid"), HID, BEAM, share, half, ids, rank, sall, out)

    return pl.pallas_call(
        place_kernel,
        out_shape=shape((qd, 2 * width // HID), F32),
        in_specs=[VM] * 3,
        out_specs=VM,
        compiler_params=pltpu.CompilerParams(vmem_limit_bytes=24 * 2**20),
        name="place",
    )(beam_ids, rank, sall)


def solution(mesh):
    return jax.shard_map(
        shards,
        mesh=mesh,
        in_specs=(
            P("beam", None),
            P("beam", None),
            P("beam", None),
            P(None, "hid"),
            P(None, "hid"),
            P(None, "hid"),
            P("hid"),
            P("hid"),
        ),
        out_specs=P("beam", "hid"),
        check_vma=False,
    )
```

```python
import functools
import math

import jax
import jax.numpy as jnp
from jax import lax
from jax.experimental import pallas as pl
from jax.experimental.pallas import tpu as pltpu
from jax.sharding import PartitionSpec as P

F32, BF16, I32 = jnp.float32, jnp.bfloat16, jnp.int32
NT = (((1,), (1,)), ((), ()))
TN = (((0,), (0,)), ((), ()))


def iota(shape, dim):
    return lax.broadcasted_iota(I32, shape, dim)


def route(h, nbeam, share, half, ranked, midway, ids_ref, req_ref, rank_ref, a_ref, c_ref, v0_ref, v1_ref, q_ref):
    qd, width = ids_ref.shape
    lo = ids_ref[:, :128]
    hi = ids_ref[:, 128:]
    ids = jnp.concatenate([lo, hi], axis=0)
    rows = ids.shape[0]
    owner = ids // half
    before_lane = (iota((128, 128), 0) < iota((128, 128), 1)).astype(BF16)
    ones = jnp.ones((128, 128), BF16)
    both = jnp.concatenate([before_lane, ones], axis=1)
    before_row = (iota((rows, rows), 1) < iota((rows, rows), 0)).astype(BF16)
    rank = jnp.zeros((rows, 128), F32)
    for o in range(nbeam):
        hit = owner == o
        counts = jnp.dot(hit.astype(BF16), both, preferred_element_type=F32)
        above = jnp.dot(before_row, counts[:, 128:].astype(BF16), preferred_element_type=F32)
        rank = rank + jnp.where(hit, counts[:, :128] + above, 0.0)
    rank = rank.astype(I32)
    rank = jnp.concatenate([rank[:qd], rank[qd:]], axis=1)
    rank_ref[...] = rank
    ranked()
    ids = ids_ref[...]
    owner = ids // half
    offset = ids - owner * half
    local = rank - h * share
    place = owner * 256 + local
    inside = (local >= 0) & (local < share)
    a_ref[...] = jnp.where(inside, place // 128, -1)
    c_ref[...] = place % 128
    v0_ref[...] = (offset % 128).astype(F32)
    v1_ref[...] = (offset // 128).astype(F32)
    q_ref[...] = iota((qd, width), 0).astype(F32)
    na = 2 * nbeam
    arow = iota((na, width), 0)
    crow = iota((128, width), 0)

    def step(r, total):
        one = pl.ds(r, 1)
        hit = arow == a_ref[one, :]
        left = jnp.concatenate([jnp.where(hit, ref[one, :], 0.0) for ref in (v0_ref, v1_ref, q_ref)], axis=0)
        right = (crow == c_ref[one, :]).astype(F32)
        return total + lax.dot_general(left.astype(BF16), right.astype(BF16), NT, preferred_element_type=F32)

    table = lax.fori_loop(0, qd // 2, step, jnp.zeros((3 * na, 128), F32), unroll=8)
    midway()
    table = lax.fori_loop(qd // 2, qd, step, table, unroll=8).astype(I32)
    offs = table[:na] + 128 * table[na : 2 * na]
    qs = table[2 * na :]
    for o in range(nbeam):
        req_ref[o, 0:2, :] = offs[2 * o : 2 * o + 2]
        req_ref[o, 2:4, :] = qs[2 * o : 2 * o + 2]


def table_copies(table_ref, buf_ref, sems):
    groups = table_ref.shape[0] // 8
    width = table_ref.shape[1]
    src = table_ref.reshape(groups, 8, width)
    dst = buf_ref.reshape(groups, 4, 2, width)
    return [pltpu.make_async_copy(src.at[:, 2 * p : 2 * p + 2, :], dst.at[:, p], sems.at[p]) for p in range(4)]


def gather(share, off_ref, buf_ref, rows_ref, first, count):
    for i in range(count):
        for k in range(share):
            rows_ref[i * share + k] = buf_ref[off_ref[first + i, k // 128, k % 128]]


def split2(x):
    hi = x.astype(BF16)
    return hi, (x - hi.astype(F32)).astype(BF16)


def score(share, b0, nb, qd, twice_ref, rows_ref, queries_ref, wq_ref, wc_ref, wx_ref, vec_ref, out_ref):
    shards = wq_ref.shape[0]
    width = queries_ref.shape[1]
    m = nb * 2 * share
    qrows = []
    for i in range(nb):
        b = b0 + i
        oht = (iota((qd, 2 * share), 0) == twice_ref[pl.ds(b, 1), :]).astype(F32).astype(BF16)
        qb = queries_ref[pl.ds(pl.multiple_of(b * qd, qd), qd), :]
        qrows.append(lax.dot_general(oht, qb, TN, preferred_element_type=F32).astype(BF16))
    qrow = jnp.concatenate(qrows, axis=0) if nb > 1 else qrows[0]
    child = rows_ref[...].reshape(m, width)
    cross = child * qrow
    acc = jnp.zeros((m, 128), F32)
    for n in range(0, shards, 2):
        pair = lambda ref: jnp.concatenate([ref[n], ref[n + 1]], axis=1)
        pre = jnp.dot(child, pair(wc_ref), preferred_element_type=F32)
        pre += jnp.dot(cross, pair(wx_ref), preferred_element_type=F32)
        pre += jnp.dot(qrow, pair(wq_ref), preferred_element_type=F32)
        for j in range(2):
            part = pre[:, 128 * j : 128 * j + 128]
            acc += jnp.maximum(part + vec_ref[n + j, 0:1, :], 0.0) * vec_ref[n + j, 1:2, :]
    total = acc.T
    total = jnp.sum(total, axis=0, keepdims=True)
    for i in range(nb):
        for t in range(2 * share // 128):
            lo = i * 2 * share + t * 128
            out_ref[pl.ds((b0 + i) * (2 * share // 128) + t, 1), :] = total[:, lo : lo + 128]


def unpermute(h, nhid, nbeam, share, half, ids_ref, rank_ref, sall_ref, out_ref):
    qd, width = ids_ref.shape
    per = width // nhid

    def own(x):
        mine = jnp.zeros((qd, per), I32)
        for k in range(nhid):
            mine = jnp.where(h == k, x[:, k * per : (k + 1) * per], mine)
        return jnp.concatenate([mine[8 * g : 8 * g + 8] for g in range(qd // 8)], axis=1)

    owner = own(ids_ref[...]) // half
    rank = own(rank_ref[...])
    chunk = rank // share
    local = rank - chunk * share
    tiles = 2 * share // 128
    row = (chunk * nbeam + owner) * tiles + local // 64
    lane = (local % 64) * 2
    nrows = nhid * nbeam * tiles
    scores = sall_ref[...].reshape(nrows, 128).T
    hi, lo = split2(scores)
    parts = jnp.concatenate([hi, lo], axis=0)
    lanes = lane.shape[1]
    rio = iota((nrows, lanes), 0)
    cio = iota((128, lanes), 0)
    evens, odds = [], []
    for i in range(8):
        onehot = (rio == row[i : i + 1]).astype(F32).astype(BF16)
        got = jnp.dot(parts, onehot, preferred_element_type=F32)
        got = got[:128] + got[128:]
        evens.append(jnp.sum(jnp.where(cio == lane[i : i + 1], got, 0.0), axis=0, keepdims=True))
        odds.append(jnp.sum(jnp.where(cio == lane[i : i + 1] + 1, got, 0.0), axis=0, keepdims=True))
    even = jnp.concatenate(split2(jnp.concatenate(evens, axis=0)), axis=0)
    odd = jnp.concatenate(split2(jnp.concatenate(odds, axis=0)), axis=0)
    n = iota((lanes, 2 * lanes), 1)
    k = iota((lanes, 2 * lanes), 0)
    mixed = jnp.dot(even, (n == 2 * k).astype(BF16), preferred_element_type=F32)
    mixed += jnp.dot(odd, (n == 2 * k + 1).astype(BF16), preferred_element_type=F32)
    mixed = mixed[:8] + mixed[8:]
    for g in range(qd // 8):
        out_ref[8 * g : 8 * g + 8, :] = mixed[:, 2 * per * g : 2 * per * (g + 1)]


BEAM, HID = 16, 8
MESH = pl.DeviceIdType.MESH
VM = pl.BlockSpec(memory_space=pltpu.VMEM)
ANY = pl.BlockSpec(memory_space=pltpu.HBM)


def shape(dims, dtype):
    return jax.ShapeDtypeStruct(dims, dtype)


def dma(*dims):
    return pltpu.SemaphoreType.DMA(dims)


def remote(src, dst, send, recv, device):
    return pltpu.make_async_remote_copy(
        src_ref=src, dst_ref=dst, send_sem=send, recv_sem=recv, device_id=device, device_id_type=MESH
    )


def loop(lo, hi, body):
    def step(i, _):
        body(i)
        return 0

    lax.fori_loop(lo, hi, step, 0)


def front_kernel(
    share,
    ids_hbm,
    queries,
    wq,
    wc,
    wx,
    bias,
    w_out,
    table,
    rank,
    req_all,
    q_all,
    w_all,
    vec_all,
    buf,
    ids,
    req,
    a_ref,
    c_ref,
    v0_ref,
    v1_ref,
    qi_ref,
    table_sem,
    own_sem,
    rsend,
    rrecv,
    qsend,
    qrecv,
    msend,
    vsend,
    vrecv,
    wsend,
    wrecv,
    psend,
    precv,
    fsend,
    frecv,
):
    b, h = lax.axis_index("beam"), lax.axis_index("hid")
    core = lax.rem(b, 2)
    mate = b + 1 - 2 * core
    z = lax.rem(h, 2)
    across = h + 1 - 2 * z
    beyond = lax.rem(b + BEAM // 2, BEAM)
    qd = ids.shape[0]
    half = table.shape[0] // 2
    depth = w_all.shape[2] // 2

    def beam_peer(j):
        return lax.rem(b + j, BEAM)

    def hid_peer(j):
        return lax.rem(h + j, HID)

    def x_peer(j):
        return lax.rem(h + 2 * j, HID)

    ids_copy = pltpu.make_async_copy(ids_hbm, ids, own_sem.at[6])
    ids_copy.start()
    barrier = pltpu.get_barrier_semaphore()
    loop(1, BEAM, lambda j: pl.semaphore_signal(barrier, inc=1, device_id=(beam_peer(j), h), device_id_type=MESH))
    loop(1, HID, lambda j: pl.semaphore_signal(barrier, inc=1, device_id=(b, hid_peer(j)), device_id_type=MESH))
    pl.semaphore_signal(barrier, inc=1, device_id=(beyond, across), device_id_type=MESH)

    def q_rows(i):
        return pl.ds(pl.multiple_of(i * qd, qd), qd)

    own = [
        pltpu.make_async_copy(src, w_all.at[h, i], own_sem.at[i]) for i, src in enumerate((wq, wc, wx))
    ]
    own.append(pltpu.make_async_copy(queries, q_all.at[q_rows(b), :], own_sem.at[3]))
    own.append(pltpu.make_async_copy(bias, vec_all.at[h, 0:1, :], own_sem.at[4]))
    own.append(pltpu.make_async_copy(w_out, vec_all.at[h, 1:2, :], own_sem.at[5]))
    for copy in own:
        copy.start()
    pulls = table_copies(table, buf, table_sem)
    for copy in pulls:
        copy.start()
    def piece(shard, part):
        return w_all.at[shard, :, pl.ds(pl.multiple_of(part * depth, depth), depth), :]

    def w_copy(shard, to, slot):
        return remote(piece(shard, core), piece(shard, core), wsend.at[slot], wrecv.at[shard], (b, to))

    def z_copy(shard):
        return remote(piece(shard, core), piece(shard, core), wsend.at[0], wrecv.at[shard], (beyond, across))

    def quarter(shard, side):
        start = pl.multiple_of(core * depth + side * (depth // 2), depth // 2)
        return w_all.at[shard, :, pl.ds(start, depth // 2), :]

    def pass_on(shard, side, lane):
        part = quarter(shard, side)
        return remote(part, part, fsend.at[lane + side], frecv.at[lane + side], (b, x_peer(3 - 2 * side)))

    beside = [x_peer(j) for j in (1, 3)]
    near = [lax.rem(across + 2 * j, HID) for j in (1, 3)]
    ends = (x_peer(2), lax.rem(across + 4, HID))

    def mate_copy(shard):
        return remote(piece(shard, core), piece(shard, core), psend.at[shard], precv.at[shard], (mate, h))

    def mate_arrival(shard):
        other = piece(shard, 1 - core)
        return remote(other, other, psend.at[shard], precv.at[shard], (mate, h))

    def q_copy(to, slot):
        return remote(q_all.at[q_rows(slot), :], q_all.at[q_rows(slot), :], qsend.at[to], qrecv.at[slot], (to, h))

    def q_mate(slot):
        return remote(q_all.at[q_rows(slot), :], q_all.at[q_rows(slot), :], msend.at[slot], qrecv.at[slot], (mate, h))

    def twin(j):
        return lax.rem(b + 2 * j, BEAM)

    def mates_twin(j):
        return lax.rem(mate + 2 * j, BEAM)

    def v_copy(to, slot):
        return remote(vec_all.at[slot], vec_all.at[slot], vsend.at[to], vrecv.at[slot], (b, to))

    def r_copy(to, slot):
        return remote(req.at[to], req_all.at[slot], rsend.at[to], rrecv.at[slot], (to, h))

    def ranked():
        for copy in own:
            copy.wait()
        pl.semaphore_wait(barrier, BEAM + HID - 1)
        z_copy(h).start()
        for j in (1, 3):
            w_copy(h, x_peer(j), j).start()
        loop(1, HID, lambda j: v_copy(hid_peer(j), h).start())
        loop(1, BEAM // 2, lambda j: q_copy(twin(j), b).start())
        q_mate(b).start()

    def midway():
        z_copy(across).wait_recv()
        for j in (1, 3):
            w_copy(across, x_peer(j), 3 + j).start()
        mate_copy(across).start()

    ids_copy.wait()
    route(h, BEAM, share, half, ranked, midway, ids, req, rank, a_ref, c_ref, v0_ref, v1_ref, qi_ref)
    loop(1, BEAM, lambda j: r_copy(beam_peer(j), b).start())
    req_all[pl.ds(b, 1)] = req[pl.ds(b, 1)]

    for side, shard in enumerate(beside):
        w_copy(shard, shard, 0).wait_recv()
        pass_on(shard, side, 0).start()
        mate_copy(shard).start()

    def hand_over(j):
        q_copy(twin(j), twin(j)).wait_recv()
        q_mate(twin(j)).start()

    loop(1, BEAM // 2, hand_over)


    for side, shard in enumerate(near):
        w_copy(shard, shard, 0).wait_recv()
        pass_on(shard, side, 2).start()
        mate_copy(shard).start()
    for i, shard in enumerate(ends):
        for side in range(2):
            pass_on(shard, side, 2 * i).wait_recv()
        mate_copy(shard).start()
    loop(1, BEAM, lambda j: r_copy(beam_peer(j), beam_peer(j)).wait_recv())
    for copy in pulls:
        copy.wait()
    loop(0, BEAM // 2, lambda j: q_mate(mates_twin(j)).wait_recv())
    loop(1, HID, lambda j: v_copy(hid_peer(j), hid_peer(j)).wait_recv())
    loop(1, HID, lambda j: mate_arrival(hid_peer(j)).wait_recv())

    z_copy(h).wait_send()
    for j in (1, 3):
        w_copy(h, x_peer(j), j).wait_send()
        w_copy(across, x_peer(j), 3 + j).wait_send()
    for i, pair in enumerate((beside, near)):
        for side, shard in enumerate(pair):
            pass_on(shard, side, 2 * i).wait_send()
    loop(1, BEAM // 2, lambda j: q_copy(twin(j), b).wait_send())
    loop(0, BEAM // 2, lambda j: q_mate(twin(j)).wait_send())
    loop(1, BEAM, lambda j: r_copy(beam_peer(j), b).wait_send())
    loop(1, HID, lambda j: v_copy(hid_peer(j), h).wait_send())
    loop(1, HID, lambda j: mate_copy(hid_peer(j)).wait_send())


def back_kernel(scores, sall, bsend, brecv, hsend, hrecv):
    b, h = lax.axis_index("beam"), lax.axis_index("hid")
    tiles = scores.shape[0] // BEAM

    def lists(i):
        return pl.ds(i * tiles, tiles)

    def beam_peer(j):
        return lax.rem(b + j, BEAM)

    def hid_peer(j):
        return lax.rem(h + j, HID)

    barrier = pltpu.get_barrier_semaphore()
    loop(1, BEAM, lambda j: pl.semaphore_signal(barrier, inc=1, device_id=(beam_peer(j), h), device_id_type=MESH))
    loop(1, HID, lambda j: pl.semaphore_signal(barrier, inc=1, device_id=(b, hid_peer(j)), device_id_type=MESH))
    pl.semaphore_wait(barrier, BEAM + HID - 2)

    def back(to, slot):
        return remote(scores.at[lists(to), :], sall.at[h, lists(slot), :], bsend.at[to], brecv.at[slot], (to, h))

    def spread(to, slot):
        return remote(sall.at[slot], sall.at[slot], hsend.at[to], hrecv.at[slot], (b, to))

    loop(1, BEAM, lambda j: back(beam_peer(j), b).start())
    for t in range(tiles):
        sall[h, pl.ds(b * tiles + t, 1), :] = scores[pl.ds(b * tiles + t, 1), :]
    loop(1, BEAM, lambda j: back(beam_peer(j), beam_peer(j)).wait_recv())
    loop(1, HID, lambda j: spread(hid_peer(j), h).start())
    loop(1, BEAM, lambda j: back(beam_peer(j), b).wait_send())
    loop(1, HID, lambda j: spread(hid_peer(j), h).wait_send())
    loop(1, HID, lambda j: spread(hid_peer(j), hid_peer(j)).wait_recv())


def score_kernel(share, nb, qd, req, off, queries, w_all, vec, buf, scores, rows, rows2, twice):
    lists = req[...]
    qs = jnp.concatenate([lists[:, 2, :], lists[:, 3, : share - 128]], axis=1).astype(F32).astype(BF16)
    dup = (iota((share, 2 * share), 1) // 2 == iota((share, 2 * share), 0)).astype(F32).astype(BF16)
    twice[...] = jnp.dot(qs, dup, preferred_element_type=F32).astype(I32)

    def run(first, now, then):
        gather(share, off, buf, then, jnp.minimum(first + nb, BEAM - nb), nb)
        score(share, first, nb, qd, twice, now, queries, w_all.at[:, 0], w_all.at[:, 1], w_all.at[:, 2], vec, scores)

    def step(i):
        run(2 * i * nb, rows, rows2)
        run((2 * i + 1) * nb, rows2, rows)

    gather(share, off, buf, rows, 0, nb)
    loop(0, BEAM // (2 * nb), step)


def shards(queries, beam_ids, child_table, w_query, w_child, w_cross, bias, w_out):
    qd, width = beam_ids.shape
    embed = queries.shape[1]
    half = child_table.shape[0] // 2
    hid_dev = w_query.shape[1]
    share = 3 * qd * width // (2 * BEAM * HID)
    nb = 2
    tiles = 2 * share // 128
    ints = pltpu.VMEM((qd, width), I32)
    floats = pltpu.VMEM((qd, width), F32)

    rank, req_all, q_all, w_all, vec_all, buf = pl.pallas_call(
        functools.partial(front_kernel, share),
        out_shape=(
            pltpu.VMEM((qd, width), I32),
            pltpu.VMEM((BEAM, 4, 128), I32),
            pltpu.VMEM((BEAM * qd, embed), BF16),
            pltpu.VMEM((HID, 3, embed, hid_dev), BF16),
            pltpu.VMEM((HID, 2, hid_dev), F32),
            pltpu.VMEM((half, 2, embed), BF16),
        ),
        in_specs=[ANY] * 8,
        out_specs=(VM,) * 6,
        scratch_shapes=[
            ints,
            pltpu.VMEM((BEAM, 4, 128), I32),
            ints,
            ints,
            floats,
            floats,
            floats,
            dma(4),
            dma(7),
            *[dma(BEAM)] * 5,
            *[dma(HID)] * 2,
            dma(7),
            dma(HID),
            *[dma(HID)] * 2,
            *[dma(4)] * 2,
        ],
        compiler_params=pltpu.CompilerParams(collective_id=0, has_side_effects=True, vmem_limit_bytes=45 * 2**20),
        name="front",
    )(beam_ids, queries, w_query, w_child, w_cross, bias.reshape(1, -1), w_out.reshape(1, -1), child_table)

    scores = pl.pallas_call(
        functools.partial(score_kernel, share, nb, qd),
        out_shape=pltpu.VMEM((BEAM * tiles, 128), F32),
        in_specs=[VM, pl.BlockSpec(memory_space=pltpu.SMEM)] + [VM] * 4,
        out_specs=VM,
        scratch_shapes=[*[pltpu.VMEM((nb * share, 2, embed), BF16)] * 2, pltpu.VMEM((BEAM, 2 * share), I32)],
        compiler_params=pltpu.CompilerParams(vmem_limit_bytes=20 * 2**20),
        name="score",
    )(req_all, req_all, q_all, w_all, vec_all, buf)

    sall = pl.pallas_call(
        back_kernel,
        out_shape=pltpu.VMEM((HID, BEAM * tiles, 128), F32),
        in_specs=[VM],
        out_specs=VM,
        scratch_shapes=[dma(BEAM), dma(BEAM), dma(HID), dma(HID)],
        compiler_params=pltpu.CompilerParams(collective_id=1, has_side_effects=True, vmem_limit_bytes=8 * 2**20),
        name="give_back",
    )(scores)

    def place_kernel(ids, rank, sall, out):
        unpermute(lax.axis_index("hid"), HID, BEAM, share, half, ids, rank, sall, out)

    return pl.pallas_call(
        place_kernel,
        out_shape=shape((qd, 2 * width // HID), F32),
        in_specs=[VM] * 3,
        out_specs=VM,
        compiler_params=pltpu.CompilerParams(vmem_limit_bytes=24 * 2**20),
        name="place",
    )(beam_ids, rank, sall)


def solution(mesh):
    return jax.shard_map(
        shards,
        mesh=mesh,
        in_specs=(
            P("beam", None),
            P("beam", None),
            P("beam", None),
            P(None, "hid"),
            P(None, "hid"),
            P(None, "hid"),
            P("hid"),
            P("hid"),
        ),
        out_specs=P("beam", "hid"),
        check_vma=False,
    )
```

```python
import functools
import math

import jax
import jax.numpy as jnp
from jax import lax
from jax.experimental import pallas as pl
from jax.experimental.pallas import tpu as pltpu
from jax.sharding import PartitionSpec as P

F32, BF16, I32 = jnp.float32, jnp.bfloat16, jnp.int32
NT = (((1,), (1,)), ((), ()))
TN = (((0,), (0,)), ((), ()))


def iota(shape, dim):
    return lax.broadcasted_iota(I32, shape, dim)


def route(h, nbeam, share, half, ranked, midway, ids_ref, req_ref, rank_ref, a_ref, c_ref, v0_ref, v1_ref, q_ref):
    qd, width = ids_ref.shape
    lo = ids_ref[:, :128]
    hi = ids_ref[:, 128:]
    ids = jnp.concatenate([lo, hi], axis=0)
    rows = ids.shape[0]
    owner = ids // half
    before_lane = (iota((128, 128), 0) < iota((128, 128), 1)).astype(BF16)
    ones = jnp.ones((128, 128), BF16)
    both = jnp.concatenate([before_lane, ones], axis=1)
    before_row = (iota((rows, rows), 1) < iota((rows, rows), 0)).astype(BF16)
    rank = jnp.zeros((rows, 128), F32)
    for o in range(nbeam):
        hit = owner == o
        counts = jnp.dot(hit.astype(BF16), both, preferred_element_type=F32)
        above = jnp.dot(before_row, counts[:, 128:].astype(BF16), preferred_element_type=F32)
        rank = rank + jnp.where(hit, counts[:, :128] + above, 0.0)
    rank = rank.astype(I32)
    rank = jnp.concatenate([rank[:qd], rank[qd:]], axis=1)
    rank_ref[...] = rank
    ranked()
    ids = ids_ref[...]
    owner = ids // half
    offset = ids - owner * half
    local = rank - h * share
    place = owner * 256 + local
    inside = (local >= 0) & (local < share)
    a_ref[...] = jnp.where(inside, place // 128, -1)
    c_ref[...] = place % 128
    v0_ref[...] = (offset % 128).astype(F32)
    v1_ref[...] = (offset // 128).astype(F32)
    q_ref[...] = iota((qd, width), 0).astype(F32)
    na = 2 * nbeam
    arow = iota((na, width), 0)
    crow = iota((128, width), 0)

    def step(r, total):
        one = pl.ds(r, 1)
        hit = arow == a_ref[one, :]
        left = jnp.concatenate([jnp.where(hit, ref[one, :], 0.0) for ref in (v0_ref, v1_ref, q_ref)], axis=0)
        right = (crow == c_ref[one, :]).astype(F32)
        return total + lax.dot_general(left.astype(BF16), right.astype(BF16), NT, preferred_element_type=F32)

    table = lax.fori_loop(0, qd // 2, step, jnp.zeros((3 * na, 128), F32), unroll=16)
    midway()
    table = lax.fori_loop(qd // 2, qd, step, table, unroll=16).astype(I32)
    offs = table[:na] + 128 * table[na : 2 * na]
    qs = table[2 * na :]
    for o in range(nbeam):
        req_ref[o, 0:2, :] = offs[2 * o : 2 * o + 2]
        req_ref[o, 2:4, :] = qs[2 * o : 2 * o + 2]


def table_copies(table_ref, buf_ref, sems):
    groups = table_ref.shape[0] // 8
    width = table_ref.shape[1]
    src = table_ref.reshape(groups, 8, width)
    dst = buf_ref.reshape(groups, 4, 2, width)
    return [pltpu.make_async_copy(src.at[:, 2 * p : 2 * p + 2, :], dst.at[:, p], sems.at[p]) for p in range(4)]


def gather(share, off_ref, buf_ref, rows_ref, first, count):
    for i in range(count):
        for k in range(share):
            rows_ref[i * share + k] = buf_ref[off_ref[first + i, k // 128, k % 128]]


def split2(x):
    hi = x.astype(BF16)
    return hi, (x - hi.astype(F32)).astype(BF16)


def score(share, b0, nb, qd, twice_ref, rows_ref, queries_ref, wq_ref, wc_ref, wx_ref, vec_ref, out_ref):
    shards = wq_ref.shape[0]
    width = queries_ref.shape[1]
    m = nb * 2 * share
    qrows = []
    for i in range(nb):
        b = b0 + i
        oht = (iota((qd, 2 * share), 0) == twice_ref[pl.ds(b, 1), :]).astype(F32).astype(BF16)
        qb = queries_ref[pl.ds(pl.multiple_of(b * qd, qd), qd), :]
        qrows.append(lax.dot_general(oht, qb, TN, preferred_element_type=F32).astype(BF16))
    qrow = jnp.concatenate(qrows, axis=0) if nb > 1 else qrows[0]
    child = rows_ref[...].reshape(m, width)
    cross = child * qrow
    acc = jnp.zeros((m, 128), F32)
    for n in range(0, shards, 2):
        pair = lambda ref: jnp.concatenate([ref[n], ref[n + 1]], axis=1)
        pre = jnp.dot(child, pair(wc_ref), preferred_element_type=F32)
        pre += jnp.dot(cross, pair(wx_ref), preferred_element_type=F32)
        pre += jnp.dot(qrow, pair(wq_ref), preferred_element_type=F32)
        for j in range(2):
            part = pre[:, 128 * j : 128 * j + 128]
            acc += jnp.maximum(part + vec_ref[n + j, 0:1, :], 0.0) * vec_ref[n + j, 1:2, :]
    total = acc.T
    total = jnp.sum(total, axis=0, keepdims=True)
    for i in range(nb):
        for t in range(2 * share // 128):
            lo = i * 2 * share + t * 128
            out_ref[pl.ds((b0 + i) * (2 * share // 128) + t, 1), :] = total[:, lo : lo + 128]


def unpermute(h, nhid, nbeam, share, half, ids_ref, rank_ref, sall_ref, out_ref):
    qd, width = ids_ref.shape
    per = width // nhid

    def own(x):
        mine = jnp.zeros((qd, per), I32)
        for k in range(nhid):
            mine = jnp.where(h == k, x[:, k * per : (k + 1) * per], mine)
        return jnp.concatenate([mine[8 * g : 8 * g + 8] for g in range(qd // 8)], axis=1)

    owner = own(ids_ref[...]) // half
    rank = own(rank_ref[...])
    chunk = rank // share
    local = rank - chunk * share
    tiles = 2 * share // 128
    row = (chunk * nbeam + owner) * tiles + local // 64
    lane = (local % 64) * 2
    nrows = nhid * nbeam * tiles
    scores = sall_ref[...].reshape(nrows, 128).T
    hi, lo = split2(scores)
    parts = jnp.concatenate([hi, lo], axis=0)
    lanes = lane.shape[1]
    rio = iota((nrows, lanes), 0)
    cio = iota((128, lanes), 0)
    evens, odds = [], []
    for i in range(8):
        onehot = (rio == row[i : i + 1]).astype(F32).astype(BF16)
        got = jnp.dot(parts, onehot, preferred_element_type=F32)
        got = got[:128] + got[128:]
        evens.append(jnp.sum(jnp.where(cio == lane[i : i + 1], got, 0.0), axis=0, keepdims=True))
        odds.append(jnp.sum(jnp.where(cio == lane[i : i + 1] + 1, got, 0.0), axis=0, keepdims=True))
    even = jnp.concatenate(split2(jnp.concatenate(evens, axis=0)), axis=0)
    odd = jnp.concatenate(split2(jnp.concatenate(odds, axis=0)), axis=0)
    n = iota((lanes, 2 * lanes), 1)
    k = iota((lanes, 2 * lanes), 0)
    mixed = jnp.dot(even, (n == 2 * k).astype(BF16), preferred_element_type=F32)
    mixed += jnp.dot(odd, (n == 2 * k + 1).astype(BF16), preferred_element_type=F32)
    mixed = mixed[:8] + mixed[8:]
    for g in range(qd // 8):
        out_ref[8 * g : 8 * g + 8, :] = mixed[:, 2 * per * g : 2 * per * (g + 1)]


BEAM, HID = 16, 8
MESH = pl.DeviceIdType.MESH
VM = pl.BlockSpec(memory_space=pltpu.VMEM)
ANY = pl.BlockSpec(memory_space=pltpu.HBM)


def shape(dims, dtype):
    return jax.ShapeDtypeStruct(dims, dtype)


def dma(*dims):
    return pltpu.SemaphoreType.DMA(dims)


def remote(src, dst, send, recv, device):
    return pltpu.make_async_remote_copy(
        src_ref=src, dst_ref=dst, send_sem=send, recv_sem=recv, device_id=device, device_id_type=MESH
    )


def loop(lo, hi, body):
    def step(i, _):
        body(i)
        return 0

    lax.fori_loop(lo, hi, step, 0)


def front_kernel(
    share,
    ids_hbm,
    queries,
    wq,
    wc,
    wx,
    bias,
    w_out,
    table,
    rank,
    req_all,
    q_all,
    w_all,
    vec_all,
    buf,
    ids,
    req,
    a_ref,
    c_ref,
    v0_ref,
    v1_ref,
    qi_ref,
    table_sem,
    own_sem,
    rsend,
    rrecv,
    qsend,
    qrecv,
    msend,
    vsend,
    vrecv,
    wsend,
    wrecv,
    psend,
    precv,
    fsend,
    frecv,
):
    b, h = lax.axis_index("beam"), lax.axis_index("hid")
    core = lax.rem(b, 2)
    mate = b + 1 - 2 * core
    z = lax.rem(h, 2)
    across = h + 1 - 2 * z
    beyond = lax.rem(b + BEAM // 2, BEAM)
    qd = ids.shape[0]
    half = table.shape[0] // 2
    depth = w_all.shape[2] // 2

    def beam_peer(j):
        return lax.rem(b + j, BEAM)

    def hid_peer(j):
        return lax.rem(h + j, HID)

    def x_peer(j):
        return lax.rem(h + 2 * j, HID)

    ids_copy = pltpu.make_async_copy(ids_hbm, ids, own_sem.at[6])
    ids_copy.start()
    barrier = pltpu.get_barrier_semaphore()
    loop(1, BEAM, lambda j: pl.semaphore_signal(barrier, inc=1, device_id=(beam_peer(j), h), device_id_type=MESH))
    loop(1, HID, lambda j: pl.semaphore_signal(barrier, inc=1, device_id=(b, hid_peer(j)), device_id_type=MESH))
    pl.semaphore_signal(barrier, inc=1, device_id=(beyond, across), device_id_type=MESH)

    def q_rows(i):
        return pl.ds(pl.multiple_of(i * qd, qd), qd)

    own = [
        pltpu.make_async_copy(src, w_all.at[h, i], own_sem.at[i]) for i, src in enumerate((wq, wc, wx))
    ]
    own.append(pltpu.make_async_copy(queries, q_all.at[q_rows(b), :], own_sem.at[3]))
    own.append(pltpu.make_async_copy(bias, vec_all.at[h, 0:1, :], own_sem.at[4]))
    own.append(pltpu.make_async_copy(w_out, vec_all.at[h, 1:2, :], own_sem.at[5]))
    for copy in own:
        copy.start()
    pulls = table_copies(table, buf, table_sem)
    for copy in pulls:
        copy.start()
    def piece(shard, part):
        return w_all.at[shard, :, pl.ds(pl.multiple_of(part * depth, depth), depth), :]

    def w_copy(shard, to, slot):
        return remote(piece(shard, core), piece(shard, core), wsend.at[slot], wrecv.at[shard], (b, to))

    def z_copy(shard):
        return remote(piece(shard, core), piece(shard, core), wsend.at[0], wrecv.at[shard], (beyond, across))

    def quarter(shard, side):
        start = pl.multiple_of(core * depth + side * (depth // 2), depth // 2)
        return w_all.at[shard, :, pl.ds(start, depth // 2), :]

    def pass_on(shard, side, lane):
        part = quarter(shard, side)
        return remote(part, part, fsend.at[lane + side], frecv.at[lane + side], (b, x_peer(3 - 2 * side)))

    beside = [x_peer(j) for j in (1, 3)]
    near = [lax.rem(across + 2 * j, HID) for j in (1, 3)]
    ends = (x_peer(2), lax.rem(across + 4, HID))

    def mate_copy(shard):
        return remote(piece(shard, core), piece(shard, core), psend.at[shard], precv.at[shard], (mate, h))

    def mate_arrival(shard):
        other = piece(shard, 1 - core)
        return remote(other, other, psend.at[shard], precv.at[shard], (mate, h))

    def q_copy(to, slot):
        return remote(q_all.at[q_rows(slot), :], q_all.at[q_rows(slot), :], qsend.at[to], qrecv.at[slot], (to, h))

    def q_mate(slot):
        return remote(q_all.at[q_rows(slot), :], q_all.at[q_rows(slot), :], msend.at[slot], qrecv.at[slot], (mate, h))

    def twin(j):
        return lax.rem(b + 2 * j, BEAM)

    def mates_twin(j):
        return lax.rem(mate + 2 * j, BEAM)

    def v_copy(to, slot):
        return remote(vec_all.at[slot], vec_all.at[slot], vsend.at[to], vrecv.at[slot], (b, to))

    def r_copy(to, slot):
        return remote(req.at[to], req_all.at[slot], rsend.at[to], rrecv.at[slot], (to, h))

    def ranked():
        for copy in own:
            copy.wait()
        pl.semaphore_wait(barrier, BEAM + HID - 1)
        z_copy(h).start()
        for j in (1, 3):
            w_copy(h, x_peer(j), j).start()
        loop(1, HID, lambda j: v_copy(hid_peer(j), h).start())
        loop(1, BEAM // 2, lambda j: q_copy(twin(j), b).start())
        q_mate(b).start()

    def midway():
        z_copy(across).wait_recv()
        for j in (1, 3):
            w_copy(across, x_peer(j), 3 + j).start()
        mate_copy(across).start()

    ids_copy.wait()
    route(h, BEAM, share, half, ranked, midway, ids, req, rank, a_ref, c_ref, v0_ref, v1_ref, qi_ref)
    loop(1, BEAM, lambda j: r_copy(beam_peer(j), b).start())
    req_all[pl.ds(b, 1)] = req[pl.ds(b, 1)]

    for side, shard in enumerate(beside):
        w_copy(shard, shard, 0).wait_recv()
        pass_on(shard, side, 0).start()
        mate_copy(shard).start()

    def hand_over(j):
        q_copy(twin(j), twin(j)).wait_recv()
        q_mate(twin(j)).start()

    loop(1, BEAM // 2, hand_over)


    for side, shard in enumerate(near):
        w_copy(shard, shard, 0).wait_recv()
        pass_on(shard, side, 2).start()
        mate_copy(shard).start()
    for i, shard in enumerate(ends):
        for side in range(2):
            pass_on(shard, side, 2 * i).wait_recv()
        mate_copy(shard).start()
    loop(1, BEAM, lambda j: r_copy(beam_peer(j), beam_peer(j)).wait_recv())
    for copy in pulls:
        copy.wait()
    loop(0, BEAM // 2, lambda j: q_mate(mates_twin(j)).wait_recv())
    loop(1, HID, lambda j: v_copy(hid_peer(j), hid_peer(j)).wait_recv())
    loop(1, HID, lambda j: mate_arrival(hid_peer(j)).wait_recv())

    z_copy(h).wait_send()
    for j in (1, 3):
        w_copy(h, x_peer(j), j).wait_send()
        w_copy(across, x_peer(j), 3 + j).wait_send()
    for i, pair in enumerate((beside, near)):
        for side, shard in enumerate(pair):
            pass_on(shard, side, 2 * i).wait_send()
    loop(1, BEAM // 2, lambda j: q_copy(twin(j), b).wait_send())
    loop(0, BEAM // 2, lambda j: q_mate(twin(j)).wait_send())
    loop(1, BEAM, lambda j: r_copy(beam_peer(j), b).wait_send())
    loop(1, HID, lambda j: v_copy(hid_peer(j), h).wait_send())
    loop(1, HID, lambda j: mate_copy(hid_peer(j)).wait_send())


def back_kernel(scores, sall, bsend, brecv, hsend, hrecv):
    b, h = lax.axis_index("beam"), lax.axis_index("hid")
    tiles = scores.shape[0] // BEAM

    def lists(i):
        return pl.ds(i * tiles, tiles)

    def beam_peer(j):
        return lax.rem(b + j, BEAM)

    def hid_peer(j):
        return lax.rem(h + j, HID)

    barrier = pltpu.get_barrier_semaphore()
    loop(1, BEAM, lambda j: pl.semaphore_signal(barrier, inc=1, device_id=(beam_peer(j), h), device_id_type=MESH))
    loop(1, HID, lambda j: pl.semaphore_signal(barrier, inc=1, device_id=(b, hid_peer(j)), device_id_type=MESH))
    pl.semaphore_wait(barrier, BEAM + HID - 2)

    def back(to, slot):
        return remote(scores.at[lists(to), :], sall.at[h, lists(slot), :], bsend.at[to], brecv.at[slot], (to, h))

    def spread(to, slot):
        return remote(sall.at[slot], sall.at[slot], hsend.at[to], hrecv.at[slot], (b, to))

    loop(1, BEAM, lambda j: back(beam_peer(j), b).start())
    for t in range(tiles):
        sall[h, pl.ds(b * tiles + t, 1), :] = scores[pl.ds(b * tiles + t, 1), :]
    loop(1, BEAM, lambda j: back(beam_peer(j), beam_peer(j)).wait_recv())
    loop(1, HID, lambda j: spread(hid_peer(j), h).start())
    loop(1, BEAM, lambda j: back(beam_peer(j), b).wait_send())
    loop(1, HID, lambda j: spread(hid_peer(j), h).wait_send())
    loop(1, HID, lambda j: spread(hid_peer(j), hid_peer(j)).wait_recv())


def score_kernel(share, nb, qd, req, off, queries, w_all, vec, buf, scores, rows, rows2, twice):
    lists = req[...]
    qs = jnp.concatenate([lists[:, 2, :], lists[:, 3, : share - 128]], axis=1).astype(F32).astype(BF16)
    dup = (iota((share, 2 * share), 1) // 2 == iota((share, 2 * share), 0)).astype(F32).astype(BF16)
    twice[...] = jnp.dot(qs, dup, preferred_element_type=F32).astype(I32)

    def run(first, now, then):
        gather(share, off, buf, then, jnp.minimum(first + nb, BEAM - nb), nb)
        score(share, first, nb, qd, twice, now, queries, w_all.at[:, 0], w_all.at[:, 1], w_all.at[:, 2], vec, scores)

    def step(i):
        run(2 * i * nb, rows, rows2)
        run((2 * i + 1) * nb, rows2, rows)

    gather(share, off, buf, rows, 0, nb)
    loop(0, BEAM // (2 * nb), step)


def shards(queries, beam_ids, child_table, w_query, w_child, w_cross, bias, w_out):
    qd, width = beam_ids.shape
    embed = queries.shape[1]
    half = child_table.shape[0] // 2
    hid_dev = w_query.shape[1]
    share = 3 * qd * width // (2 * BEAM * HID)
    nb = 2
    tiles = 2 * share // 128
    ints = pltpu.VMEM((qd, width), I32)
    floats = pltpu.VMEM((qd, width), F32)

    rank, req_all, q_all, w_all, vec_all, buf = pl.pallas_call(
        functools.partial(front_kernel, share),
        out_shape=(
            pltpu.VMEM((qd, width), I32),
            pltpu.VMEM((BEAM, 4, 128), I32),
            pltpu.VMEM((BEAM * qd, embed), BF16),
            pltpu.VMEM((HID, 3, embed, hid_dev), BF16),
            pltpu.VMEM((HID, 2, hid_dev), F32),
            pltpu.VMEM((half, 2, embed), BF16),
        ),
        in_specs=[ANY] * 8,
        out_specs=(VM,) * 6,
        scratch_shapes=[
            ints,
            pltpu.VMEM((BEAM, 4, 128), I32),
            ints,
            ints,
            floats,
            floats,
            floats,
            dma(4),
            dma(7),
            *[dma(BEAM)] * 5,
            *[dma(HID)] * 2,
            dma(7),
            dma(HID),
            *[dma(HID)] * 2,
            *[dma(4)] * 2,
        ],
        compiler_params=pltpu.CompilerParams(collective_id=0, has_side_effects=True, vmem_limit_bytes=45 * 2**20),
        name="front",
    )(beam_ids, queries, w_query, w_child, w_cross, bias.reshape(1, -1), w_out.reshape(1, -1), child_table)

    scores = pl.pallas_call(
        functools.partial(score_kernel, share, nb, qd),
        out_shape=pltpu.VMEM((BEAM * tiles, 128), F32),
        in_specs=[VM, pl.BlockSpec(memory_space=pltpu.SMEM)] + [VM] * 4,
        out_specs=VM,
        scratch_shapes=[*[pltpu.VMEM((nb * share, 2, embed), BF16)] * 2, pltpu.VMEM((BEAM, 2 * share), I32)],
        compiler_params=pltpu.CompilerParams(vmem_limit_bytes=20 * 2**20),
        name="score",
    )(req_all, req_all, q_all, w_all, vec_all, buf)

    sall = pl.pallas_call(
        back_kernel,
        out_shape=pltpu.VMEM((HID, BEAM * tiles, 128), F32),
        in_specs=[VM],
        out_specs=VM,
        scratch_shapes=[dma(BEAM), dma(BEAM), dma(HID), dma(HID)],
        compiler_params=pltpu.CompilerParams(collective_id=1, has_side_effects=True, vmem_limit_bytes=8 * 2**20),
        name="give_back",
    )(scores)

    def place_kernel(ids, rank, sall, out):
        unpermute(lax.axis_index("hid"), HID, BEAM, share, half, ids, rank, sall, out)

    return pl.pallas_call(
        place_kernel,
        out_shape=shape((qd, 2 * width // HID), F32),
        in_specs=[VM] * 3,
        out_specs=VM,
        compiler_params=pltpu.CompilerParams(vmem_limit_bytes=24 * 2**20),
        name="place",
    )(beam_ids, rank, sall)


def solution(mesh):
    return jax.shard_map(
        shards,
        mesh=mesh,
        in_specs=(
            P("beam", None),
            P("beam", None),
            P("beam", None),
            P(None, "hid"),
            P(None, "hid"),
            P(None, "hid"),
            P("hid"),
            P("hid"),
        ),
        out_specs=P("beam", "hid"),
        check_vma=False,
    )
```
